16 devices in a mesh: tp: 2 (over z), dp: 8 (over y, x, core).
Axes of the slice: x: 2, y: 2, z: 2, core: 2. Of those that a mesh axis runs over, the one named last changes fastest.
Arguments:
- hid_q: bfloat16 [256, 512, 2048], P('dp')
- hid_d: bfloat16 [16, 512, 2048], P('dp')
- len_q: int32 [256], P('dp')
- len_d: int32 [16], P('dp')
- pos_doc: int32 [256], P('dp')
- w_q: bfloat16 [2048, 2048], P(None, 'tp')
- w_k: bfloat16 [2048, 1024], P(None, 'tp')
- w_v: bfloat16 [2048, 1024], P(None, 'tp')
- w_o: bfloat16 [2048, 2048], P('tp')
- w_gate: bfloat16 [2048, 6144], P(None, 'tp')
- w_up: bfloat16 [2048, 6144], P(None, 'tp')
- w_down: bfloat16 [6144, 2048], P('tp')
- g_in: bfloat16 [2048], replicated
- g_q: bfloat16 [128], replicated
- g_k: bfloat16 [128], replicated
- g_post: bfloat16 [2048], replicated
- g_final: bfloat16 [2048], replicated
Outputs:
- output 1: float32 [256], P('dp')
- output 2: bfloat16 [256, 512, 2048], P('dp')
- output 3: bfloat16 [16, 512, 2048], P('dp')
- output 4: float32 [2048, 2048], P(None, 'tp')
- output 5: float32 [2048, 1024], P(None, 'tp')
- output 6: float32 [2048, 1024], P(None, 'tp')
- output 7: float32 [2048, 2048], P('tp')
- output 8: float32 [2048, 6144], P(None, 'tp')
- output 9: float32 [2048, 6144], P(None, 'tp')
- output 10: float32 [6144, 2048], P('tp')
- output 11: float32 [2048], replicated
- output 12: float32 [128], replicated
- output 13: float32 [128], replicated
- output 14: float32 [2048], replicated
- output 15: float32 [2048], replicated
All inputs are finite; a program needn't handle non-finite values.
Results may differ from the reference program's by a relative error of at most 0.02.
Values sent between devices are 32-bit elements.
A program may use at most 1.25 GiB of HBM per device.

```python
import jax
import jax.numpy as jnp
from jax import lax

N_QRY = 256
N_DOC = 16
SEQ_LEN = 512
D_MODEL = 2048
HEADS = 16
KV_HEADS = 8
HEAD_DIM = 128
FF_DIM = 6144

NORM_EPS = 1e-6
ROPE_THETA = 1000000.0
TEMPERATURE = 0.05
POS_MIX = 0.3


def dense_init(rng_key, fan_in, fan_out):
    return (jax.random.normal(rng_key, (fan_in, fan_out), jnp.float32) * fan_in ** -0.5).astype(jnp.bfloat16)


def gain_init(rng_key, n_width):
    return (1.0 + 0.3 * jax.random.normal(rng_key, (n_width,), jnp.float32)).astype(jnp.bfloat16)


def setup_inputs(seed: int = 0) -> dict:
    rng_keys = jax.random.split(jax.random.key(seed), 17)
    q_max = SEQ_LEN // 4
    len_q = jax.random.randint(rng_keys[0], (N_QRY,), 1, q_max + 1).at[0].set(q_max).at[1].set(1)
    len_d = jax.random.randint(rng_keys[1], (N_DOC,), 1, SEQ_LEN + 1).at[0].set(SEQ_LEN).at[1].set(1)
    pos_doc = jax.random.randint(rng_keys[2], (N_QRY,), 0, N_DOC).at[0].set(N_DOC - 1).at[1].set(0)
    hid_d = jax.random.normal(rng_keys[3], (N_DOC, SEQ_LEN, D_MODEL), jnp.float32)
    hid_q = jax.random.normal(rng_keys[4], (N_QRY, SEQ_LEN, D_MODEL), jnp.float32)
    target = hid_d[pos_doc, len_d[pos_doc] - 1]
    at_last = (jnp.arange(SEQ_LEN)[None, :] == (len_q - 1)[:, None])[:, :, None]
    mixed_q = (1.0 - POS_MIX ** 2) ** 0.5 * hid_q + POS_MIX * target[:, None, :]
    hid_q = jnp.where(at_last, mixed_q, hid_q)
    q_width = HEADS * HEAD_DIM
    kv_width = KV_HEADS * HEAD_DIM
    return {
        'hid_q': hid_q.astype(jnp.bfloat16),
        'hid_d': hid_d.astype(jnp.bfloat16),
        'len_q': len_q,
        'len_d': len_d,
        'pos_doc': pos_doc,
        'w_q': dense_init(rng_keys[5], D_MODEL, q_width),
        'w_k': dense_init(rng_keys[6], D_MODEL, kv_width),
        'w_v': dense_init(rng_keys[7], D_MODEL, kv_width),
        'w_o': dense_init(rng_keys[8], q_width, D_MODEL),
        'w_gate': dense_init(rng_keys[9], D_MODEL, FF_DIM),
        'w_up': dense_init(rng_keys[10], D_MODEL, FF_DIM),
        'w_down': dense_init(rng_keys[11], FF_DIM, D_MODEL),
        'g_in': gain_init(rng_keys[12], D_MODEL),
        'g_q': gain_init(rng_keys[13], HEAD_DIM),
        'g_k': gain_init(rng_keys[14], HEAD_DIM),
        'g_post': gain_init(rng_keys[15], D_MODEL),
        'g_final': gain_init(rng_keys[16], D_MODEL),
    }


def as_bf16(values):
    return values.astype(jnp.bfloat16).astype(jnp.float32)


def norm_rows(values, gain_vec):
    return values * lax.rsqrt(jnp.mean(values * values, axis=-1, keepdims=True) + NORM_EPS) * gain_vec


def rotate(values, angles):
    half_dim = values.shape[-1] // 2
    first_half = values[..., :half_dim]
    second_half = values[..., half_dim:]
    cos_a = jnp.cos(angles)
    sin_a = jnp.sin(angles)
    return jnp.concatenate([first_half * cos_a - second_half * sin_a, second_half * cos_a + first_half * sin_a], axis=-1)


def attend(q_raw, k_raw, v_raw, g_q, g_k, lens):
    n_seq, seq_len, kv_width = k_raw.shape
    n_kv = kv_width // HEAD_DIM
    group_size = q_raw.shape[1] // kv_width
    inv_freq = ROPE_THETA ** (-jnp.arange(0, HEAD_DIM, 2).astype(jnp.float32) / HEAD_DIM)
    key_angle = jnp.arange(seq_len).astype(jnp.float32)[:, None] * inv_freq
    key_rot = norm_rows(k_raw.reshape(n_seq, seq_len, n_kv, HEAD_DIM), g_k)
    key_rot = as_bf16(rotate(key_rot, key_angle[None, :, None, :]))
    q_angle = (lens - 1).astype(jnp.float32)[:, None] * inv_freq
    query_rot = norm_rows(q_raw.reshape(n_seq, n_kv, group_size, HEAD_DIM), g_q)
    query_rot = as_bf16(rotate(query_rot, q_angle[:, None, None, :]))
    scores = jnp.einsum('nkgd,nskd->nkgs', query_rot, key_rot) * HEAD_DIM ** -0.5
    key_valid = jnp.arange(seq_len)[None, :] < lens[:, None]
    scores = jnp.where(key_valid[:, None, None, :], scores, -1e30)
    attn_prob = as_bf16(jax.nn.softmax(scores, axis=-1))
    val_heads = v_raw.reshape(n_seq, seq_len, n_kv, HEAD_DIM)
    attn_mix = jnp.einsum('nkgs,nskd->nkgd', attn_prob, val_heads)
    return as_bf16(attn_mix).reshape(n_seq, q_raw.shape[1])


def embed(hidden, lens, weights):
    w_q, w_k, w_v, w_o, w_gate, w_up, w_down, g_in, g_q, g_k, g_post, g_final = weights
    n_seq, seq_len, model_width = hidden.shape
    x_norm = as_bf16(norm_rows(hidden, g_in))
    x_flat = x_norm.reshape(n_seq * seq_len, model_width)
    k_raw = as_bf16(jnp.dot(x_flat, w_k)).reshape(n_seq, seq_len, -1)
    v_raw = as_bf16(jnp.dot(x_flat, w_v)).reshape(n_seq, seq_len, -1)
    last_idx = (lens - 1)[:, None, None]
    x_last = jnp.take_along_axis(x_norm, last_idx, axis=1)[:, 0]
    h_last = jnp.take_along_axis(hidden, last_idx, axis=1)[:, 0]
    q_raw = as_bf16(jnp.dot(x_last, w_q))
    h_mid = h_last + jnp.dot(attend(q_raw, k_raw, v_raw, g_q, g_k, lens), w_o)
    y_norm = as_bf16(norm_rows(h_mid, g_post))
    gate_val = as_bf16(jnp.dot(y_norm, w_gate))
    up_val = as_bf16(jnp.dot(y_norm, w_up))
    hidden_act = as_bf16(jax.nn.silu(gate_val) * up_val)
    h_out = h_mid + jnp.dot(hidden_act, w_down)
    z_norm = norm_rows(h_out, g_final)
    return z_norm * lax.rsqrt(jnp.sum(z_norm * z_norm, axis=-1, keepdims=True))


def contrast_rows(hid_q, hid_d, len_q, len_d, pos_doc, weights):
    emb_q = embed(hid_q, len_q, weights)
    emb_d = embed(hid_d, len_d, weights)
    logits = jnp.dot(emb_q, emb_d.T) / TEMPERATURE
    log_norm = jax.nn.logsumexp(logits, axis=1)
    pos_logit = jnp.take_along_axis(logits, pos_doc[:, None], axis=1)[:, 0]
    return log_norm - pos_logit


def reference(hid_q, hid_d, len_q, len_d, pos_doc, w_q, w_k, w_v, w_o, w_gate, w_up, w_down, g_in, g_q, g_k, g_post, g_final):
    weights = tuple(weight_in.astype(jnp.float32) for weight_in in (w_q, w_k, w_v, w_o, w_gate, w_up, w_down, g_in, g_q, g_k, g_post, g_final))

    def loss_of(q_float, d_float, weights_f):
        row_losses = contrast_rows(q_float, d_float, len_q, len_d, pos_doc, weights_f)
        return jnp.mean(row_losses), row_losses

    mean_loss, pull_back, loss_rows = jax.vjp(loss_of, hid_q.astype(jnp.float32), hid_d.astype(jnp.float32), weights, has_aux=True)
    d_hid_q, d_hid_d, d_w = pull_back(jnp.ones_like(mean_loss))
    return (loss_rows, d_hid_q.astype(jnp.bfloat16), d_hid_d.astype(jnp.bfloat16), d_w[0], d_w[1], d_w[2], d_w[3], d_w[4], d_w[5], d_w[6], d_w[7], d_w[8], d_w[9], d_w[10], d_w[11])
```

```python
import functools
import jax
import jax.numpy as jnp
from jax import lax
from jax.experimental import pallas as pl
from jax.experimental.pallas import tpu as pltpu
from jax.sharding import PartitionSpec as P

NORM_EPS = 1e-6
ROPE_THETA = 1000000.0
TEMPERATURE = 0.05
HEAD = 128
Q_MAX = 128
BF = jnp.bfloat16
F32 = jnp.float32
SWAP = [(0, 1), (1, 0)]
VMEM = 60 * 1024 * 1024


def norm_rows(values, gain_vec):
    return values * lax.rsqrt(jnp.mean(values * values, axis=-1, keepdims=True) + NORM_EPS) * gain_vec


def norm_back(values, gain_vec, d_out):
    scale = lax.rsqrt(jnp.mean(values * values, axis=-1, keepdims=True) + NORM_EPS)
    g_dout = d_out * gain_vec
    d_values = scale * g_dout - values * scale ** 3 * jnp.mean(values * g_dout, axis=-1, keepdims=True)
    d_gain = jnp.sum((d_out * values * scale).reshape(-1, values.shape[-1]), axis=0)
    return d_values, d_gain


def rope_tables(positions):
    inv_freq = ROPE_THETA ** (-jnp.arange(0, HEAD, 2, dtype=F32) / HEAD)
    angles = positions.astype(F32)[:, None] * inv_freq
    cos_a, sin_a = jnp.cos(angles), jnp.sin(angles)
    return jnp.concatenate([cos_a, cos_a], axis=-1), jnp.concatenate([-sin_a, sin_a], axis=-1)


def rotate_query(q_raw, g_q, cos_t, sin_t):
    n_seq = q_raw.shape[0]
    normed = norm_rows(q_raw.reshape(n_seq, -1, HEAD).astype(F32), g_q)
    half = HEAD // 2
    swapped = jnp.concatenate([normed[..., half:], normed[..., :half]], axis=-1)
    return (normed * cos_t[:, None, :] + swapped * sin_t[:, None, :]).astype(BF)


def head_mask(n_rows, width):
    row_head = lax.broadcasted_iota(jnp.int32, (n_rows, width), 0) // 2
    lane_head = lax.broadcasted_iota(jnp.int32, (n_rows, width), 1) // HEAD
    return row_head == lane_head


def block_diag(per_head):
    n_seq, n_q, _ = per_head.shape
    n_kv = n_q // 2
    wide = jnp.tile(per_head, (1, 1, n_kv))
    wide = jnp.where(head_mask(n_q, n_kv * HEAD)[None], wide, jnp.zeros_like(wide))
    return jnp.pad(wide, ((0, 0), (0, 16 - n_q), (0, 0)))


def take_diag(wide):
    kept = jnp.where(head_mask(wide.shape[0], wide.shape[1]), wide, 0.0)
    total = kept[:, :HEAD]
    for head in range(1, wide.shape[1] // HEAD):
        total = total + kept[:, head * HEAD:(head + 1) * HEAD]
    return total


def key_stats(k_raw):
    k_f = k_raw.astype(F32)
    scale = lax.rsqrt(jnp.mean(k_f * k_f, axis=-1, keepdims=True) + NORM_EPS)
    return k_f * scale, scale


def turn(values, cos_t, sin_t):
    return values * cos_t + pltpu.roll(values, HEAD // 2, 1) * sin_t


def variants(max_len, sizes, body):
    low = 0
    for size in sizes:
        pl.when(jnp.logical_and(max_len > low, max_len <= size))(functools.partial(body, size))
        low = size


NT = (((1,), (1,)), ((), ()))
TN = (((0,), (0,)), ((), ()))


def fwd_body(do_norm, group, sizes, order_ref, lens_ref, *refs):
    h_refs, refs = refs[:group if do_norm else 1], refs[group if do_norm else 1:]
    if do_norm:
        gin_ref, w_ref, qbd_ref, gk_ref, cos_ref, sin_ref, x_ref, kv_ref, p_ref, o_ref = refs
        for g in range(group):
            hid = h_refs[g][0].astype(F32)
            scale = lax.rsqrt(jnp.mean(hid * hid, axis=-1, keepdims=True) + NORM_EPS)
            x_ref[g] = (hid * scale * gin_ref[...]).astype(BF)
    else:
        w_ref, qbd_ref, gk_ref, cos_ref, sin_ref, kv_ref, p_ref, o_ref = refs
        x_ref = h_refs[0]
    width = w_ref.shape[1]
    kv_half = width // 2
    step = pl.program_id(0)

    def run(size):
        def project(j, carry):
            cols = pl.ds(pl.multiple_of(j * 256, 256), 256)
            x_val = x_ref[:, :size, :].reshape(group * size, x_ref.shape[2])
            out = jnp.dot(x_val, w_ref[:, cols], preferred_element_type=F32)
            kv_ref[:, :size, cols] = out.astype(BF).reshape(group, size, 256)
            return carry

        lax.fori_loop(0, width // 256, project, 0)
        cos_t, sin_t = cos_ref[:size], sin_ref[:size]
        for g in range(group):
            length = lens_ref[step * group + g]
            k_rot = []
            for head in range(kv_half // HEAD):
                k_hat, _ = key_stats(kv_ref[g, :size, head * HEAD:(head + 1) * HEAD])
                k_rot.append(turn(k_hat * gk_ref[...], cos_t, sin_t).astype(BF))
            k_rot = jnp.concatenate(k_rot, axis=-1)
            scores = lax.dot_general(qbd_ref[g], k_rot, NT, preferred_element_type=F32) * HEAD ** -0.5
            valid = lax.broadcasted_iota(jnp.int32, scores.shape, 1) < length
            scores = jnp.where(valid, scores, -1e30)
            expd = jnp.exp(scores - jnp.max(scores, axis=-1, keepdims=True))
            prob = expd / jnp.sum(expd, axis=-1, keepdims=True)
            p_ref[g, :, :size] = prob
            mix = jnp.dot(prob.astype(BF), kv_ref[g, :size, kv_half:], preferred_element_type=F32)
            o_ref[g] = take_diag(mix)

    variants(lens_ref[step * group + group - 1], sizes, run)


def attn_fwd(hid_or_x, order, lens, rows, group, sizes, w_kv, qbd, g_k, cos_t, sin_t, g_in=None):
    n_seq, width = order.shape[0], w_kv.shape[1]
    model = w_kv.shape[0]
    do_norm = g_in is not None
    once = dict(pipeline_mode=pl.Buffered(buffer_count=1))
    by_group = lambda *shape: pl.BlockSpec((group,) + shape, lambda i, o, l: (i,) + (0,) * len(shape))
    whole = lambda arr: pl.BlockSpec(arr.shape, lambda i, o, l: (0,) * arr.ndim, **once)
    if do_norm:
        in_specs = [pl.BlockSpec((1, rows, model), lambda i, o, l, g=g: (o[i * group + g], 0, 0)) for g in range(group)]
        operands = [hid_or_x] * group + [g_in]
        in_specs.append(whole(g_in))
    else:
        in_specs, operands = [by_group(rows, model)], [hid_or_x]
    in_specs += [whole(w_kv), by_group(16, width // 2), whole(g_k), whole(cos_t), whole(sin_t)]
    operands += [w_kv, qbd, g_k, cos_t, sin_t]
    out_specs = [by_group(rows, width), by_group(16, rows), by_group(16, HEAD)]
    out_shape = [jax.ShapeDtypeStruct((n_seq, rows, width), BF), jax.ShapeDtypeStruct((n_seq, 16, rows), F32), jax.ShapeDtypeStruct((n_seq, 16, HEAD), F32)]
    if do_norm:
        out_specs.insert(0, by_group(rows, model))
        out_shape.insert(0, jax.ShapeDtypeStruct((n_seq, rows, model), BF))
    return pl.pallas_call(
        functools.partial(fwd_body, do_norm, group, sizes),
        grid_spec=pltpu.PrefetchScalarGridSpec(num_scalar_prefetch=2, grid=(n_seq // group,), in_specs=in_specs, out_specs=out_specs),
        out_shape=out_shape,
        compiler_params=pltpu.CompilerParams(dimension_semantics=("arbitrary",), vmem_limit_bytes=VMEM),
        cost_estimate=pl.CostEstimate(flops=2 * n_seq * rows * model * width, bytes_accessed=n_seq * rows * model * 4, transcendentals=0),
        name="attn_fwd" + ("_norm" if do_norm else "") + str(rows),
    )(order, lens, *operands)


def bwd_body(group, sizes, lens_ref, kv_ref, p_ref, qbd_ref, dobd_ref, gk_ref, cos_ref, sin_ref, dkv_ref, dq_ref, dgk_ref):
    step = pl.program_id(0)
    rows, width = kv_ref.shape[1], kv_ref.shape[2]
    kv_half = width // 2

    @pl.when(step == 0)
    def _():
        dgk_ref[...] = jnp.zeros_like(dgk_ref)

    def run(size):
        cos_t, sin_t = cos_ref[:size], sin_ref[:size]
        gk = gk_ref[...]
        for g in range(group):
            prob = p_ref[g, :, :size]
            qbd, dobd = qbd_ref[g], dobd_ref[g]
            d_prob = lax.dot_general(dobd, kv_ref[g, :size, kv_half:], NT, preferred_element_type=F32)
            d_prob = d_prob.astype(BF).astype(F32)
            d_score = prob * (d_prob - jnp.sum(prob * d_prob, axis=-1, keepdims=True))
            d_score = (d_score * HEAD ** -0.5).astype(BF)
            d_key = lax.dot_general(d_score, qbd, TN, preferred_element_type=F32)
            d_val = lax.dot_general(prob.astype(BF), dobd, TN, preferred_element_type=F32)
            dkv_ref[g, :size, kv_half:] = d_val.astype(BF)
            k_rot = []
            d_gain = jnp.zeros((size, HEAD), F32)
            for head in range(kv_half // HEAD):
                lanes = slice(head * HEAD, (head + 1) * HEAD)
                k_hat, scale = key_stats(kv_ref[g, :size, lanes])
                k_rot.append(turn(k_hat * gk, cos_t, sin_t).astype(BF))
                d_norm = turn(d_key[:, lanes].astype(BF).astype(F32), cos_t, -sin_t)
                d_gain = d_gain + d_norm * k_hat
                d_hat = d_norm * gk
                d_raw = scale * (d_hat - k_hat * jnp.mean(k_hat * d_hat, axis=-1, keepdims=True))
                dkv_ref[g, :size, lanes] = d_raw.astype(BF)
            d_query = jnp.dot(d_score, jnp.concatenate(k_rot, axis=-1), preferred_element_type=F32)
            dq_ref[g] = take_diag(d_query)
            dgk_ref[...] += jnp.sum(d_gain.reshape(size // 8, 8, HEAD), axis=0)
            if size < rows:
                dkv_ref[g, size:, :] = jnp.zeros((rows - size, width), BF)

    variants(lens_ref[step * group + group - 1], sizes, run)


def attn_bwd(lens, group, sizes, kv, prob, qbd, dobd, g_k, cos_t, sin_t):
    n_seq, rows, width = kv.shape
    once = dict(pipeline_mode=pl.Buffered(buffer_count=1))
    by_group = lambda *shape: pl.BlockSpec((group,) + shape, lambda i, l: (i,) + (0,) * len(shape))
    whole = lambda arr: pl.BlockSpec(arr.shape, lambda i, l: (0,) * arr.ndim, **once)
    return pl.pallas_call(
        functools.partial(bwd_body, group, sizes),
        grid_spec=pltpu.PrefetchScalarGridSpec(
            num_scalar_prefetch=1, grid=(n_seq // group,),
            in_specs=[by_group(rows, width), by_group(16, rows), by_group(16, width // 2), by_group(16, width // 2), whole(g_k), whole(cos_t), whole(sin_t)],
            out_specs=[by_group(rows, width), by_group(16, HEAD), pl.BlockSpec((8, HEAD), lambda i, l: (0, 0))]),
        out_shape=[jax.ShapeDtypeStruct(kv.shape, BF), jax.ShapeDtypeStruct((n_seq, 16, HEAD), F32), jax.ShapeDtypeStruct((8, HEAD), F32)],
        compiler_params=pltpu.CompilerParams(dimension_semantics=("arbitrary",), vmem_limit_bytes=VMEM),
        cost_estimate=pl.CostEstimate(flops=20 * 1000 * n_seq * rows * width // 8, bytes_accessed=n_seq * rows * width * 4, transcendentals=0),
        name="attn_bwd" + str(rows),
    )(lens, kv, prob, qbd, dobd, g_k, cos_t, sin_t)


def dx_body(group, sizes, order_ref, lens_ref, dkv_ref, dkv2_ref, w_ref, w2_ref, h_ref, gin_ref, dxl_ref, dhm_ref, out_ref, dgin_ref, dx_ref):
    step = pl.program_id(0)
    rows, model = h_ref.shape[1], h_ref.shape[2]
    width = w_ref.shape[1]
    length = lens_ref[step]
    inner = lax.rem(step, group)

    @pl.when(step == 0)
    def _():
        dgin_ref[...] = jnp.zeros_like(dgin_ref)

    def run(size):
        @pl.when(inner == 0)
        def _():
            def project(j, carry):
                cols = pl.ds(pl.multiple_of(j * 256, 256), 256)
                d_own = dkv_ref[:, :size, :].reshape(group * size, width)
                part = lax.dot_general(d_own, w_ref[cols, :], NT, preferred_element_type=F32)
                dx_ref[:, :size, cols] = part.reshape(group, size, 256)
                return carry

            def project_other(j, carry):
                cols = pl.ds(pl.multiple_of(j * 256, 256), 256)
                d_oth = dkv2_ref[:, :size, :].reshape(group * size, width)
                part = lax.dot_general(d_oth, w2_ref[cols, :], NT, preferred_element_type=F32)
                dx_ref[:, :size, cols] += part.reshape(group, size, 256)
                return carry

            lax.fori_loop(0, model // 256, project, 0)
            lax.fori_loop(0, model // 256, project_other, 0)

        chunk = 32
        gin = gin_ref[...]

        def finish(c, carry):
            start = pl.multiple_of(c * chunk, chunk)
            here = pl.ds(start, chunk)
            hid = h_ref[0, here, :].astype(F32)
            at_last = lax.broadcasted_iota(jnp.int32, (chunk, 1), 0) + start == length - 1
            d_x = dx_ref[inner, here, :] + jnp.where(at_last, dxl_ref[0], 0.0)
            scale = lax.rsqrt(jnp.mean(hid * hid, axis=-1, keepdims=True) + NORM_EPS)
            h_hat = hid * scale
            dgin_ref[...] += jnp.sum((d_x * h_hat).reshape(chunk // 8, 8, model), axis=0)
            g_dx = d_x * gin
            d_hid = scale * (g_dx - h_hat * jnp.mean(h_hat * g_dx, axis=-1, keepdims=True))
            out_ref[0, here, :] = (d_hid + jnp.where(at_last, dhm_ref[0], 0.0)).astype(BF)
            return carry

        lax.fori_loop(0, size // chunk, finish, 0)
        if size < out_ref.shape[1]:
            out_ref[0, size:, :] = jnp.zeros((out_ref.shape[1] - size, model), BF)

    variants(lens_ref[step - inner + group - 1], sizes, run)


def attn_dx(hid, order, lens, rows, group, sizes, dkv, dkv2, w_kv, w_kv2, g_in, d_xlast, d_hmid):
    n_seq, seq_len, model = hid.shape
    width = w_kv.shape[1]
    once = dict(pipeline_mode=pl.Buffered(buffer_count=1))
    by_group = lambda *shape: pl.BlockSpec((group,) + shape, lambda i, o, l: (i // group,) + (0,) * len(shape))
    whole = lambda arr: pl.BlockSpec(arr.shape, lambda i, o, l: (0,) * arr.ndim, **once)
    one_row = pl.BlockSpec((1, 1, model), lambda i, o, l: (i, 0, 0))
    return pl.pallas_call(
        functools.partial(dx_body, group, sizes),
        grid_spec=pltpu.PrefetchScalarGridSpec(
            num_scalar_prefetch=2, grid=(n_seq,),
            in_specs=[by_group(rows, width), by_group(rows, width), whole(w_kv), whole(w_kv2),
                      pl.BlockSpec((1, rows, model), lambda i, o, l: (o[i], 0, 0)), whole(g_in), one_row, one_row],
            out_specs=[pl.BlockSpec((1, seq_len, model), lambda i, o, l: (o[i], 0, 0)), pl.BlockSpec((8, model), lambda i, o, l: (0, 0))],
            scratch_shapes=[pltpu.VMEM((group, rows, model), F32)]),
        out_shape=[jax.ShapeDtypeStruct(hid.shape, BF), jax.ShapeDtypeStruct((8, model), F32)],
        compiler_params=pltpu.CompilerParams(dimension_semantics=("arbitrary",), vmem_limit_bytes=VMEM),
        cost_estimate=pl.CostEstimate(flops=4 * n_seq * rows * model * width, bytes_accessed=hid.size * 4, transcendentals=0),
        name="attn_dx" + str(rows),
    )(order, lens, dkv, dkv2, w_kv, w_kv2, hid, g_in, d_xlast[:, None, :], d_hmid[:, None, :])


def wide(values):
    return values.astype(F32)


def narrow(values, unit):
    return (values * unit).astype(BF)


def swap_tp(values):
    return lax.ppermute(values, 'tp', SWAP)


def psum_tp(values):
    return values + swap_tp(values)


def swiglu(gate_in, up_in):
    return jax.nn.silu(gate_in) * up_in


def final_head(h_out, g_final):
    z_norm = norm_rows(h_out, g_final)
    return z_norm * lax.rsqrt(jnp.sum(z_norm * z_norm, axis=-1, keepdims=True))


def dot(a, b):
    return jnp.dot(a, b, preferred_element_type=F32)


def dot_nt(a, b):
    return lax.dot_general(a, b, NT, preferred_element_type=F32)


def dot_tn(a, b):
    return lax.dot_general(a, b, TN, preferred_element_type=F32)


Q_SIZES = (32, 64, 96, 128)
D_SIZES = (128, 256, 384, 512)


def solution(mesh):
    dp_size = mesh.shape['dp']

    def device_step(hid_q, hid_d, len_q, len_d, pos_doc, w_q, w_k, w_v, w_o, w_gate, w_up, w_down, g_in, g_q, g_k, g_post, g_final):
        g_in, g_q, g_k, g_post, g_final = (gain.astype(F32) for gain in (g_in, g_q, g_k, g_post, g_final))
        n_q, n_d = hid_q.shape[0], hid_d.shape[0]
        seq_len = hid_q.shape[1]
        n_query = n_q * dp_size

        ids = jnp.arange(n_q)
        before = (len_q[None, :] < len_q[:, None]) | ((len_q[None, :] == len_q[:, None]) & (ids[None, :] < ids[:, None]))
        rank = jnp.sum(before, axis=1)
        is_rank = rank[None, :] == ids[:, None]
        order_q = jnp.sum(jnp.where(is_rank, ids[None, :], 0), axis=1).astype(jnp.int32)
        lens_q = jnp.sum(jnp.where(is_rank, len_q[None, :], 0), axis=1).astype(jnp.int32)
        pos_sorted = jnp.sum(jnp.where(is_rank, pos_doc[None, :], 0), axis=1).astype(jnp.int32)
        order_d = jnp.arange(n_d, dtype=jnp.int32)
        lens = jnp.concatenate([lens_q, len_d])
        unit = jnp.minimum(len_d[0], 1).astype(F32)

        w_kv = jnp.concatenate([w_k, w_v], axis=1)
        slab_rows = w_kv.shape[0] // dp_size
        slab = lax.dynamic_slice_in_dim(w_kv, lax.axis_index('dp') * slab_rows, slab_rows, axis=0)
        w_kv2 = narrow(lax.all_gather(swap_tp(wide(slab)), 'dp', axis=0, tiled=True), unit)

        h_last = jnp.concatenate([hid_q[order_q, lens_q - 1], hid_d[order_d, len_d - 1]], axis=0).astype(F32)
        x_last = norm_rows(h_last, g_in).astype(BF)
        q_raw = dot(x_last, w_q).astype(BF)
        q_cos, q_sin = rope_tables(lens - 1)
        q_rot, q_pull = jax.vjp(lambda raw, gain: rotate_query(raw, gain, q_cos, q_sin), q_raw, g_q)
        q_rot2 = narrow(swap_tp(wide(q_rot)), unit)
        qbd, qbd2 = block_diag(q_rot), block_diag(q_rot2)

        cos_t, sin_t = rope_tables(jnp.arange(seq_len))
        cos_q, sin_q = cos_t[:Q_MAX], sin_t[:Q_MAX]
        gin_row, gk_row = g_in[None, :], g_k[None, :]
        x_q, kv_q, p_q, o_q = attn_fwd(hid_q, order_q, lens_q, Q_MAX, 4, Q_SIZES, w_kv, qbd[:n_q], gk_row, cos_q, sin_q, gin_row)
        x_d, kv_d, p_d, o_d = attn_fwd(hid_d, order_d, len_d, seq_len, 1, D_SIZES, w_kv, qbd[n_q:], gk_row, cos_t, sin_t, gin_row)
        attn_out = jnp.concatenate([o_q, o_d], axis=0)[:, :q_rot.shape[1]].astype(BF).reshape(n_q + n_d, -1)

        h_mid = h_last + psum_tp(dot(attn_out, w_o))
        y_norm = norm_rows(h_mid, g_post).astype(BF)
        gate_val = dot(y_norm, w_gate).astype(BF)
        up_val = dot(y_norm, w_up).astype(BF)
        hidden_act, act_pull = jax.vjp(swiglu, gate_val.astype(F32), up_val.astype(F32))
        h_out = h_mid + psum_tp(dot(hidden_act.astype(BF), w_down))
        emb, head_pull = jax.vjp(final_head, h_out, g_final)
        emb_q, emb_d = emb[:n_q], emb[n_q:]

        all_docs = lax.all_gather(emb_d, 'dp', axis=0, tiled=True)
        logits = jnp.einsum('qd,kd->qk', emb_q, all_docs, precision=lax.Precision.HIGHEST) / TEMPERATURE
        log_norm = jax.nn.logsumexp(logits, axis=1)
        is_pos = jnp.arange(all_docs.shape[0])[None, :] == pos_sorted[:, None]
        loss_sorted = log_norm - jnp.sum(jnp.where(is_pos, logits, 0.0), axis=1)
        loss_rows = jnp.sum(jnp.where(is_rank, loss_sorted[:, None], 0.0), axis=0)
        d_logits = (jnp.exp(logits - log_norm[:, None]) - is_pos.astype(F32)) / (n_query * TEMPERATURE)
        d_emb_q = jnp.einsum('qk,kd->qd', d_logits, all_docs, precision=lax.Precision.HIGHEST)
        d_docs = jnp.einsum('qk,qd->kd', d_logits, emb_q, precision=lax.Precision.HIGHEST)
        d_emb_d = lax.psum_scatter(d_docs, 'dp', scatter_dimension=0, tiled=True)

        d_hout, d_gfinal = head_pull(jnp.concatenate([d_emb_q, d_emb_d], axis=0))
        d_hout_b = d_hout.astype(BF)
        d_act = dot_nt(d_hout_b, w_down).astype(BF)
        d_gate, d_up = act_pull(d_act.astype(F32))
        d_y = psum_tp(dot_nt(d_gate.astype(BF), w_gate) + dot_nt(d_up.astype(BF), w_up))
        d_ymid, d_gpost = norm_back(h_mid, g_post, d_y)
        d_hmid = d_hout + d_ymid
        d_hmid_b = d_hmid.astype(BF)
        d_attn = dot_nt(d_hmid_b, w_o).astype(BF).reshape(q_rot.shape)
        d_attn2 = narrow(swap_tp(wide(d_attn)), unit)
        dobd, dobd2 = block_diag(d_attn), block_diag(d_attn2)

        dkv_q, dq_q, dgk_q = attn_bwd(lens_q, 4, Q_SIZES, kv_q, p_q, qbd[:n_q], dobd[:n_q], gk_row, cos_q, sin_q)
        dkv_d, dq_d, dgk_d = attn_bwd(len_d, 1, D_SIZES, kv_d, p_d, qbd[n_q:], dobd[n_q:], gk_row, cos_t, sin_t)
        flat = lambda arr: arr.reshape(-1, arr.shape[-1])
        d_wkv = lax.psum(dot_tn(flat(x_q), flat(dkv_q)) + dot_tn(flat(x_d), flat(dkv_d)), 'dp')
        d_qrot = jnp.concatenate([dq_q, dq_d], axis=0)[:, :q_rot.shape[1]].astype(BF)
        d_qraw, d_gq = q_pull(d_qrot)
        d_xlast = psum_tp(dot_nt(d_qraw, w_q))

        kv2_q, p2_q, _ = attn_fwd(x_q, order_q, lens_q, Q_MAX, 4, Q_SIZES, w_kv2, qbd2[:n_q], gk_row, cos_q, sin_q)
        kv2_d, p2_d, _ = attn_fwd(x_d, order_d, len_d, seq_len, 1, D_SIZES, w_kv2, qbd2[n_q:], gk_row, cos_t, sin_t)
        dkv2_q, _, _ = attn_bwd(lens_q, 4, Q_SIZES, kv2_q, p2_q, qbd2[:n_q], dobd2[:n_q], gk_row, cos_q, sin_q)
        dkv2_d, _, _ = attn_bwd(len_d, 1, D_SIZES, kv2_d, p2_d, qbd2[n_q:], dobd2[n_q:], gk_row, cos_t, sin_t)
        d_hid_q, dgin_q = attn_dx(hid_q, order_q, lens_q, Q_MAX, 4, Q_SIZES, dkv_q, dkv2_q, w_kv, w_kv2, gin_row, d_xlast[:n_q], d_hmid[:n_q])
        d_hid_d, dgin_d = attn_dx(hid_d, order_d, len_d, seq_len, 1, D_SIZES, dkv_d, dkv2_d, w_kv, w_kv2, gin_row, d_xlast[n_q:], d_hmid[n_q:])

        gather = lambda arr: narrow(lax.all_gather(wide(arr), 'dp', axis=0, tiled=True), unit)
        width = h_last.shape[1]
        x_last_all = gather(x_last)
        y_attn = gather(jnp.concatenate([y_norm, attn_out], axis=1))
        y_all, attn_all = y_attn[:, :width], y_attn[:, width:]
        d_both = gather(jnp.concatenate([d_hout_b, d_hmid_b], axis=1))
        d_hout_all, d_hmid_all = d_both[:, :width], d_both[:, width:]
        d_qraw_all = gather(d_qraw)
        act_all, act_all_pull = jax.vjp(swiglu, dot(y_all, w_gate).astype(BF).astype(F32), dot(y_all, w_up).astype(BF).astype(F32))
        d_gate_all, d_up_all = act_all_pull(dot_nt(d_hout_all, w_down).astype(BF).astype(F32))
        d_wdown = dot_tn(act_all.astype(BF), d_hout_all)
        d_wgate = dot_tn(y_all, d_gate_all.astype(BF))
        d_wup = dot_tn(y_all, d_up_all.astype(BF))
        d_wo = dot_tn(attn_all, d_hmid_all)
        d_wq = dot_tn(x_last_all, d_qraw_all)

        d_gk = jnp.sum(dgk_q + dgk_d, axis=0)
        d_gin = jnp.sum(dgin_q + dgin_d, axis=0)
        gains = lax.psum(jnp.concatenate([d_gin * 0.5, d_gpost * 0.5, d_gfinal * 0.5, d_gq, d_gk]), ('tp', 'dp'))
        d_gin, d_gpost, d_gfinal = gains[:width], gains[width:2 * width], gains[2 * width:3 * width]
        d_gq, d_gk = gains[3 * width:3 * width + HEAD], gains[3 * width + HEAD:]
        kv_half = w_k.shape[1]
        return (loss_rows, d_hid_q, d_hid_d, d_wq, d_wkv[:, :kv_half], d_wkv[:, kv_half:], d_wo, d_wgate, d_wup, d_wdown,
                d_gin, d_gq, d_gk, d_gpost, d_gfinal)

    col_split = P(None, 'tp')
    row_split = P('tp', None)
    in_specs = (P('dp'), P('dp'), P('dp'), P('dp'), P('dp'), col_split, col_split, col_split, row_split, col_split, col_split, row_split, P(), P(), P(), P(), P())
    out_specs = (P('dp'), P('dp'), P('dp'), col_split, col_split, col_split, row_split, col_split, col_split, row_split, P(), P(), P(), P(), P())
    return jax.shard_map(device_step, mesh=mesh, in_specs=in_specs, out_specs=out_specs, check_vma=False)
```

```python
import functools
import jax
import jax.numpy as jnp
from jax import lax
from jax.experimental import pallas as pl
from jax.experimental.pallas import tpu as pltpu
from jax.sharding import PartitionSpec as P

NORM_EPS = 1e-6
ROPE_THETA = 1000000.0
TEMPERATURE = 0.05
HEAD = 128
Q_MAX = 128
BF = jnp.bfloat16
F32 = jnp.float32
SWAP = [(0, 1), (1, 0)]
VMEM = 60 * 1024 * 1024


def norm_rows(values, gain_vec):
    return values * lax.rsqrt(jnp.mean(values * values, axis=-1, keepdims=True) + NORM_EPS) * gain_vec


def norm_back(values, gain_vec, d_out):
    scale = lax.rsqrt(jnp.mean(values * values, axis=-1, keepdims=True) + NORM_EPS)
    g_dout = d_out * gain_vec
    d_values = scale * g_dout - values * scale ** 3 * jnp.mean(values * g_dout, axis=-1, keepdims=True)
    d_gain = jnp.sum((d_out * values * scale).reshape(-1, values.shape[-1]), axis=0)
    return d_values, d_gain


def rope_tables(positions):
    inv_freq = ROPE_THETA ** (-jnp.arange(0, HEAD, 2, dtype=F32) / HEAD)
    angles = positions.astype(F32)[:, None] * inv_freq
    cos_a, sin_a = jnp.cos(angles), jnp.sin(angles)
    return jnp.concatenate([cos_a, cos_a], axis=-1), jnp.concatenate([-sin_a, sin_a], axis=-1)


def rotate_query(q_raw, g_q, cos_t, sin_t):
    n_seq = q_raw.shape[0]
    normed = norm_rows(q_raw.reshape(n_seq, -1, HEAD).astype(F32), g_q)
    half = HEAD // 2
    swapped = jnp.concatenate([normed[..., half:], normed[..., :half]], axis=-1)
    return (normed * cos_t[:, None, :] + swapped * sin_t[:, None, :]).astype(BF)


def head_mask(n_rows, width):
    row_head = lax.rem(lax.broadcasted_iota(jnp.int32, (n_rows, width), 0), 16) // 2
    lane_head = lax.broadcasted_iota(jnp.int32, (n_rows, width), 1) // HEAD
    return row_head == lane_head


def block_diag(per_head):
    n_seq, n_q, _ = per_head.shape
    n_kv = n_q // 2
    wide = jnp.tile(per_head, (1, 1, n_kv))
    wide = jnp.where(head_mask(n_q, n_kv * HEAD)[None], wide, jnp.zeros_like(wide))
    return jnp.pad(wide, ((0, 0), (0, 16 - n_q), (0, 0)))


def take_diag(wide):
    kept = jnp.where(head_mask(wide.shape[0], wide.shape[1]), wide, 0.0)
    total = kept[:, :HEAD]
    for head in range(1, wide.shape[1] // HEAD):
        total = total + kept[:, head * HEAD:(head + 1) * HEAD]
    return total


def key_stats(k_raw):
    k_f = k_raw.astype(F32)
    scale = lax.rsqrt(jnp.mean(k_f * k_f, axis=-1, keepdims=True) + NORM_EPS)
    return k_f * scale, scale


def turn(values, cos_t, sin_t):
    return values * cos_t + pltpu.roll(values, HEAD // 2, 1) * sin_t


def variants(max_len, sizes, body):
    low = 0
    for size in sizes:
        pl.when(jnp.logical_and(max_len > low, max_len <= size))(functools.partial(body, size))
        low = size


NT = (((1,), (1,)), ((), ()))
TN = (((0,), (0,)), ((), ()))


def stacked(parts):
    return parts[0] if len(parts) == 1 else jnp.concatenate(parts, axis=0)


def row_lengths(lens_ref, first, group, shape):
    row_seq = lax.broadcasted_iota(jnp.int32, shape, 0) // 16
    lengths = jnp.full(shape, lens_ref[first], jnp.int32)
    for g in range(1, group):
        lengths = jnp.where(row_seq == g, lens_ref[first + g], lengths)
    return lengths


def fwd_body(do_norm, group, sizes, order_ref, lens_ref, *refs):
    h_refs, refs = refs[:group if do_norm else 1], refs[group if do_norm else 1:]
    if do_norm:
        gin_ref, wk_ref, wv_ref, qbd_ref, gk_ref, cos_ref, sin_ref, x_ref, kv_ref, p_ref, o_ref, rot_ref = refs
        for g in range(group):
            def norm_chunk(c, carry, g=g):
                here = pl.ds(pl.multiple_of(c * 32, 32), 32)
                hid = h_refs[g][0, here, :].astype(F32)
                scale = lax.rsqrt(jnp.mean(hid * hid, axis=-1, keepdims=True) + NORM_EPS)
                x_ref[g, here, :] = (hid * scale * gin_ref[...]).astype(BF)
                return carry

            lax.fori_loop(0, x_ref.shape[1] // 32, norm_chunk, 0)
    else:
        wk_ref, wv_ref, qbd_ref, gk_ref, cos_ref, sin_ref, kv_ref, p_ref, o_ref, rot_ref = refs
        x_ref = h_refs[0]
    kv_half = wk_ref.shape[1]
    step = pl.program_id(0)

    def run(size):
        for at, w_ref in ((0, wk_ref), (kv_half, wv_ref)):
            x_val = x_ref[:, :size, :].reshape(group * size, x_ref.shape[2])
            out = jnp.dot(x_val, w_ref[...], preferred_element_type=F32)
            kv_ref[:, :size, at:at + kv_half] = out.astype(BF).reshape(group, size, kv_half)
        cos_t, sin_t = cos_ref[:size], sin_ref[:size]
        for g in range(group):
            for head in range(kv_half // HEAD):
                lanes = slice(head * HEAD, (head + 1) * HEAD)
                k_hat, _ = key_stats(kv_ref[g, :size, lanes])
                rot_ref[g, :size, lanes] = turn(k_hat * gk_ref[...], cos_t, sin_t).astype(BF)
        scores = stacked([lax.dot_general(qbd_ref[g], rot_ref[g, :size, :], NT, preferred_element_type=F32) for g in range(group)])
        valid = lax.broadcasted_iota(jnp.int32, scores.shape, 1) < row_lengths(lens_ref, step * group, group, scores.shape)
        scores = jnp.where(valid, scores * HEAD ** -0.5, -1e30)
        expd = jnp.exp(scores - jnp.max(scores, axis=-1, keepdims=True))
        prob = expd / jnp.sum(expd, axis=-1, keepdims=True)
        p_ref[:, :, :size] = prob.reshape(group, 16, size)
        prob = prob.astype(BF)
        mix = stacked([jnp.dot(prob[g * 16:(g + 1) * 16], kv_ref[g, :size, kv_half:], preferred_element_type=F32) for g in range(group)])
        o_ref[...] = take_diag(mix).reshape(group, 16, HEAD)

    variants(lens_ref[step * group + group - 1], sizes, run)


def attn_fwd(hid_or_x, order, lens, rows, group, sizes, w_k, w_v, qbd, g_k, cos_t, sin_t, g_in=None):
    n_seq, width = order.shape[0], 2 * w_k.shape[1]
    model = w_k.shape[0]
    do_norm = g_in is not None
    once = dict(pipeline_mode=pl.Buffered(buffer_count=1))
    by_group = lambda *shape: pl.BlockSpec((group,) + shape, lambda i, o, l: (i,) + (0,) * len(shape))
    whole = lambda arr: pl.BlockSpec(arr.shape, lambda i, o, l: (0,) * arr.ndim, **once)
    if do_norm:
        in_specs = [pl.BlockSpec((1, rows, model), lambda i, o, l, g=g: (o[i * group + g], 0, 0)) for g in range(group)]
        operands = [hid_or_x] * group + [g_in]
        in_specs.append(whole(g_in))
    else:
        in_specs, operands = [by_group(rows, model)], [hid_or_x]
    in_specs += [whole(w_k), whole(w_v), by_group(16, width // 2), whole(g_k), whole(cos_t), whole(sin_t)]
    operands += [w_k, w_v, qbd, g_k, cos_t, sin_t]
    out_specs = [by_group(rows, width), by_group(16, rows), by_group(16, HEAD)]
    out_shape = [jax.ShapeDtypeStruct((n_seq, rows, width), BF), jax.ShapeDtypeStruct((n_seq, 16, rows), F32), jax.ShapeDtypeStruct((n_seq, 16, HEAD), F32)]
    if do_norm:
        out_specs.insert(0, by_group(rows, model))
        out_shape.insert(0, jax.ShapeDtypeStruct((n_seq, rows, model), BF))
    return pl.pallas_call(
        functools.partial(fwd_body, do_norm, group, sizes),
        grid_spec=pltpu.PrefetchScalarGridSpec(num_scalar_prefetch=2, grid=(n_seq // group,), in_specs=in_specs, out_specs=out_specs,
                                              scratch_shapes=[pltpu.VMEM((group, rows, width // 2), BF)]),
        out_shape=out_shape,
        compiler_params=pltpu.CompilerParams(dimension_semantics=("arbitrary",), vmem_limit_bytes=VMEM),
        cost_estimate=pl.CostEstimate(flops=2 * n_seq * rows * model * width, bytes_accessed=n_seq * rows * model * 4, transcendentals=0),
        name="attn_fwd" + ("_norm" if do_norm else "") + str(rows),
    )(order, lens, *operands)


def bwd_body(group, sizes, lens_ref, kv_ref, p_ref, qbd_ref, dobd_ref, gk_ref, cos_ref, sin_ref, dkv_ref, dq_ref, dgk_ref, rot_ref, dkey_ref):
    step = pl.program_id(0)
    rows, width = kv_ref.shape[1], kv_ref.shape[2]
    kv_half = width // 2

    @pl.when(step == 0)
    def _():
        dgk_ref[...] = jnp.zeros_like(dgk_ref)

    def run(size):
        cos_t, sin_t = cos_ref[:size], sin_ref[:size]
        gk = gk_ref[...]
        prob = p_ref[:, :, :size].reshape(group * 16, size)
        d_prob = stacked([lax.dot_general(dobd_ref[g], kv_ref[g, :size, kv_half:], NT, preferred_element_type=F32) for g in range(group)])
        d_prob = d_prob.astype(BF).astype(F32)
        d_score = prob * (d_prob - jnp.sum(prob * d_prob, axis=-1, keepdims=True))
        d_score = (d_score * HEAD ** -0.5).astype(BF)
        prob = prob.astype(BF)
        for g in range(group):
            d_key = lax.dot_general(d_score[g * 16:(g + 1) * 16], qbd_ref[g], TN, preferred_element_type=F32)
            dkey_ref[g, :size, :] = d_key.astype(BF)
            d_val = lax.dot_general(prob[g * 16:(g + 1) * 16], dobd_ref[g], TN, preferred_element_type=F32)
            dkv_ref[g, :size, kv_half:] = d_val.astype(BF)
        d_gain = jnp.zeros((8, HEAD), F32)
        for g in range(group):
            for head in range(kv_half // HEAD):
                lanes = slice(head * HEAD, (head + 1) * HEAD)
                k_hat, scale = key_stats(kv_ref[g, :size, lanes])
                rot_ref[g, :size, lanes] = turn(k_hat * gk, cos_t, sin_t).astype(BF)
                d_norm = turn(dkey_ref[g, :size, lanes].astype(F32), cos_t, -sin_t)
                d_gain = d_gain + jnp.sum((d_norm * k_hat).reshape(size // 8, 8, HEAD), axis=0)
                d_hat = d_norm * gk
                d_raw = scale * (d_hat - k_hat * jnp.mean(k_hat * d_hat, axis=-1, keepdims=True))
                dkv_ref[g, :size, lanes] = d_raw.astype(BF)
        dgk_ref[...] += d_gain
        d_query = stacked([jnp.dot(d_score[g * 16:(g + 1) * 16], rot_ref[g, :size, :], preferred_element_type=F32) for g in range(group)])
        dq_ref[...] = take_diag(d_query).reshape(group, 16, HEAD)
        if size < rows:
            dkv_ref[:, size:, :] = jnp.zeros((group, rows - size, width), BF)

    variants(lens_ref[step * group + group - 1], sizes, run)


def attn_bwd(lens, group, sizes, kv, prob, qbd, dobd, g_k, cos_t, sin_t):
    n_seq, rows, width = kv.shape
    once = dict(pipeline_mode=pl.Buffered(buffer_count=1))
    by_group = lambda *shape: pl.BlockSpec((group,) + shape, lambda i, l: (i,) + (0,) * len(shape))
    whole = lambda arr: pl.BlockSpec(arr.shape, lambda i, l: (0,) * arr.ndim, **once)
    return pl.pallas_call(
        functools.partial(bwd_body, group, sizes),
        grid_spec=pltpu.PrefetchScalarGridSpec(
            num_scalar_prefetch=1, grid=(n_seq // group,),
            in_specs=[by_group(rows, width), by_group(16, rows), by_group(16, width // 2), by_group(16, width // 2), whole(g_k), whole(cos_t), whole(sin_t)],
            out_specs=[by_group(rows, width), by_group(16, HEAD), pl.BlockSpec((8, HEAD), lambda i, l: (0, 0))],
            scratch_shapes=[pltpu.VMEM((group, rows, width // 2), BF)] * 2),
        out_shape=[jax.ShapeDtypeStruct(kv.shape, BF), jax.ShapeDtypeStruct((n_seq, 16, HEAD), F32), jax.ShapeDtypeStruct((8, HEAD), F32)],
        compiler_params=pltpu.CompilerParams(dimension_semantics=("arbitrary",), vmem_limit_bytes=VMEM),
        cost_estimate=pl.CostEstimate(flops=20 * 1000 * n_seq * rows * width // 8, bytes_accessed=n_seq * rows * width * 4, transcendentals=0),
        name="attn_bwd" + str(rows),
    )(lens, kv, prob, qbd, dobd, g_k, cos_t, sin_t)


def dx_body(group, sizes, order_ref, lens_ref, dkv_ref, dkv2_ref, wk_ref, wv_ref, wk2_ref, wv2_ref, h_ref, gin_ref, dxl_ref, dhm_ref, out_ref, dgin_ref, dx_ref):
    step = pl.program_id(0)
    rows, model = h_ref.shape[1], h_ref.shape[2]
    kv_half = wk_ref.shape[1]
    last = lens_ref[step] - 1
    inner = lax.rem(step, group)
    wide_cols = 512

    @pl.when(step == 0)
    def _():
        dgin_ref[...] = jnp.zeros_like(dgin_ref)

    def run(size):
        @pl.when(inner == 0)
        def _():
            def project(d_ref, w_refs, add, j, carry):
                cols = pl.ds(pl.multiple_of(j * wide_cols, wide_cols), wide_cols)
                part = None
                for half, w_ref in enumerate(w_refs):
                    d_half = d_ref[:, :size, half * kv_half:(half + 1) * kv_half].reshape(group * size, kv_half)
                    term = lax.dot_general(d_half, w_ref[cols, :], NT, preferred_element_type=F32)
                    part = term if part is None else part + term
                part = part.reshape(group, size, wide_cols)
                dx_ref[:, :size, cols] = dx_ref[:, :size, cols] + part if add else part
                return carry

            lax.fori_loop(0, model // wide_cols, functools.partial(project, dkv_ref, (wk_ref, wv_ref), False), 0)
            lax.fori_loop(0, model // wide_cols, functools.partial(project, dkv2_ref, (wk2_ref, wv2_ref), True), 0)

        dx_ref[inner, pl.ds(last, 1), :] += dxl_ref[0]
        chunk = 32
        tiles = [slice(t, t + HEAD) for t in range(0, model, HEAD)]

        def finish(c, carry):
            start = pl.multiple_of(c * chunk, chunk)
            here = pl.ds(start, chunk)
            at_last = lax.broadcasted_iota(jnp.int32, (chunk, HEAD), 0) + start == last
            squares, cross = jnp.zeros((chunk, HEAD), F32), jnp.zeros((chunk, HEAD), F32)
            for t in tiles:
                hid = h_ref[0, here, t].astype(F32)
                squares = squares + hid * hid
                cross = cross + hid * (dx_ref[inner, here, t] * gin_ref[:, t])
            scale = lax.rsqrt(jnp.sum(squares, axis=-1, keepdims=True) / model + NORM_EPS)
            slope = scale * scale * scale * (jnp.sum(cross, axis=-1, keepdims=True) / model)
            for t in tiles:
                hid = h_ref[0, here, t].astype(F32)
                d_x = dx_ref[inner, here, t] * scale
                dgin_ref[:, t] += jnp.sum((d_x * hid).reshape(chunk // 8, 8, HEAD), axis=0)
                d_hid = d_x * gin_ref[:, t] - hid * slope
                out_ref[0, here, t] = (d_hid + jnp.where(at_last, dhm_ref[0][:, t], 0.0)).astype(BF)
            return carry

        lax.fori_loop(0, size // chunk, finish, 0)
        if size < out_ref.shape[1]:
            out_ref[0, size:, :] = jnp.zeros((out_ref.shape[1] - size, model), BF)

    variants(lens_ref[step - inner + group - 1], sizes, run)


def attn_dx(hid, order, lens, rows, group, sizes, dkv, dkv2, w_own, w_oth, g_in, d_xlast, d_hmid):
    n_seq, seq_len, model = hid.shape
    width = dkv.shape[-1]
    once = dict(pipeline_mode=pl.Buffered(buffer_count=1))
    by_group = lambda *shape: pl.BlockSpec((group,) + shape, lambda i, o, l: (i // group,) + (0,) * len(shape))
    whole = lambda arr: pl.BlockSpec(arr.shape, lambda i, o, l: (0,) * arr.ndim, **once)
    one_row = pl.BlockSpec((1, 1, model), lambda i, o, l: (i, 0, 0))
    weights = tuple(w_own) + tuple(w_oth)
    return pl.pallas_call(
        functools.partial(dx_body, group, sizes),
        grid_spec=pltpu.PrefetchScalarGridSpec(
            num_scalar_prefetch=2, grid=(n_seq,),
            in_specs=[by_group(rows, width), by_group(rows, width)] + [whole(w) for w in weights] +
                     [pl.BlockSpec((1, rows, model), lambda i, o, l: (o[i], 0, 0)), whole(g_in), one_row, one_row],
            out_specs=[pl.BlockSpec((1, seq_len, model), lambda i, o, l: (o[i], 0, 0)), pl.BlockSpec((8, model), lambda i, o, l: (0, 0))],
            scratch_shapes=[pltpu.VMEM((group, rows, model), F32)]),
        out_shape=[jax.ShapeDtypeStruct(hid.shape, BF), jax.ShapeDtypeStruct((8, model), F32)],
        compiler_params=pltpu.CompilerParams(dimension_semantics=("arbitrary",), vmem_limit_bytes=VMEM),
        cost_estimate=pl.CostEstimate(flops=4 * n_seq * rows * model * width, bytes_accessed=hid.size * 4, transcendentals=0),
        name="attn_dx" + str(rows),
    )(order, lens, dkv, dkv2, *weights, hid, g_in, d_xlast[:, None, :], d_hmid[:, None, :])


def wide(values):
    return values.astype(F32)


def narrow(values, unit):
    return (values * unit).astype(BF)


def swap_tp(values):
    return lax.ppermute(values, 'tp', SWAP)


def psum_tp(values):
    return values + swap_tp(values)


def swiglu(gate_in, up_in):
    return jax.nn.silu(gate_in) * up_in


def final_head(h_out, g_final):
    z_norm = norm_rows(h_out, g_final)
    return z_norm * lax.rsqrt(jnp.sum(z_norm * z_norm, axis=-1, keepdims=True))


def dot(a, b):
    return jnp.dot(a, b, preferred_element_type=F32)


def dot_nt(a, b):
    return lax.dot_general(a, b, NT, preferred_element_type=F32)


def dot_tn(a, b):
    return lax.dot_general(a, b, TN, preferred_element_type=F32)


Q_SIZES = (32, 64, 96, 128)
D_SIZES = (128, 256, 384, 512)


def solution(mesh):
    dp_size = mesh.shape['dp']

    def device_step(hid_q, hid_d, len_q, len_d, pos_doc, w_q, w_k, w_v, w_o, w_gate, w_up, w_down, g_in, g_q, g_k, g_post, g_final):
        g_in, g_q, g_k, g_post, g_final = (gain.astype(F32) for gain in (g_in, g_q, g_k, g_post, g_final))
        n_q, n_d = hid_q.shape[0], hid_d.shape[0]
        seq_len = hid_q.shape[1]
        n_query = n_q * dp_size

        ids = jnp.arange(n_q)
        before = (len_q[None, :] < len_q[:, None]) | ((len_q[None, :] == len_q[:, None]) & (ids[None, :] < ids[:, None]))
        rank = jnp.sum(before, axis=1)
        is_rank = rank[None, :] == ids[:, None]
        order_q = jnp.sum(jnp.where(is_rank, ids[None, :], 0), axis=1).astype(jnp.int32)
        lens_q = jnp.sum(jnp.where(is_rank, len_q[None, :], 0), axis=1).astype(jnp.int32)
        pos_sorted = jnp.sum(jnp.where(is_rank, pos_doc[None, :], 0), axis=1).astype(jnp.int32)
        order_d = jnp.arange(n_d, dtype=jnp.int32)
        lens = jnp.concatenate([lens_q, len_d])
        unit = jnp.minimum(len_d[0], 1).astype(F32)

        kv_half = w_k.shape[1]
        slab_rows = w_k.shape[0] // dp_size
        my_slab = lambda arr: lax.dynamic_slice_in_dim(arr, lax.axis_index('dp') * slab_rows, slab_rows, axis=0)
        slab = jnp.concatenate([my_slab(w_k), my_slab(w_v)], axis=1)
        w_kv2 = narrow(lax.all_gather(swap_tp(wide(slab)), 'dp', axis=0, tiled=True), unit)
        w_k2, w_v2 = w_kv2[:, :kv_half], w_kv2[:, kv_half:]

        h_last = jnp.concatenate([hid_q[order_q, lens_q - 1], hid_d[order_d, len_d - 1]], axis=0).astype(F32)
        x_last = norm_rows(h_last, g_in).astype(BF)
        q_raw = dot(x_last, w_q).astype(BF)
        q_cos, q_sin = rope_tables(lens - 1)
        q_rot, q_pull = jax.vjp(lambda raw, gain: rotate_query(raw, gain, q_cos, q_sin), q_raw, g_q)
        q_rot2 = narrow(swap_tp(wide(q_rot)), unit)
        qbd, qbd2 = block_diag(q_rot), block_diag(q_rot2)

        cos_t, sin_t = rope_tables(jnp.arange(seq_len))
        cos_q, sin_q = cos_t[:Q_MAX], sin_t[:Q_MAX]
        gin_row, gk_row = g_in[None, :], g_k[None, :]
        x_q, kv_q, p_q, o_q = attn_fwd(hid_q, order_q, lens_q, Q_MAX, 4, Q_SIZES, w_k, w_v, qbd[:n_q], gk_row, cos_q, sin_q, gin_row)
        x_d, kv_d, p_d, o_d = attn_fwd(hid_d, order_d, len_d, seq_len, 1, D_SIZES, w_k, w_v, qbd[n_q:], gk_row, cos_t, sin_t, gin_row)
        attn_out = jnp.concatenate([o_q, o_d], axis=0)[:, :q_rot.shape[1]].astype(BF).reshape(n_q + n_d, -1)
        attn_out, w_k2, w_v2 = lax.optimization_barrier((attn_out, w_k2, w_v2))

        h_mid = h_last + psum_tp(dot(attn_out, w_o))
        y_norm = norm_rows(h_mid, g_post).astype(BF)
        width = h_last.shape[1]
        gather = lambda arr: narrow(lax.all_gather(wide(arr), 'dp', axis=0, tiled=True), unit)
        early = gather(jnp.concatenate([x_last, y_norm, attn_out], axis=1))
        gate_val = dot(y_norm, w_gate).astype(BF)
        up_val = dot(y_norm, w_up).astype(BF)
        hidden_act, act_pull = jax.vjp(swiglu, gate_val.astype(F32), up_val.astype(F32))
        h_out = h_mid + psum_tp(dot(hidden_act.astype(BF), w_down))
        emb, head_pull = jax.vjp(final_head, h_out, g_final)
        emb_q, emb_d = emb[:n_q], emb[n_q:]

        all_docs = lax.all_gather(emb_d, 'dp', axis=0, tiled=True)
        logits = jnp.einsum('qd,kd->qk', emb_q, all_docs, precision=lax.Precision.HIGHEST) / TEMPERATURE
        log_norm = jax.nn.logsumexp(logits, axis=1)
        is_pos = jnp.arange(all_docs.shape[0])[None, :] == pos_sorted[:, None]
        loss_sorted = log_norm - jnp.sum(jnp.where(is_pos, logits, 0.0), axis=1)
        loss_rows = jnp.sum(jnp.where(is_rank, loss_sorted[:, None], 0.0), axis=0)
        d_logits = (jnp.exp(logits - log_norm[:, None]) - is_pos.astype(F32)) / (n_query * TEMPERATURE)
        d_emb_q = jnp.einsum('qk,kd->qd', d_logits, all_docs, precision=lax.Precision.HIGHEST)
        d_docs = jnp.einsum('qk,qd->kd', d_logits, emb_q, precision=lax.Precision.HIGHEST)
        d_docs = lax.all_to_all(d_docs, 'dp', 0, 0, tiled=True)
        d_emb_d = jnp.sum(d_docs.reshape(dp_size, n_d, width), axis=0)

        d_hout, d_gfinal = head_pull(jnp.concatenate([d_emb_q, d_emb_d], axis=0))
        d_hout_b = d_hout.astype(BF)
        d_act = dot_nt(d_hout_b, w_down).astype(BF)
        d_gate, d_up = act_pull(d_act.astype(F32))
        d_y = psum_tp(dot_nt(d_gate.astype(BF), w_gate) + dot_nt(d_up.astype(BF), w_up))
        d_ymid, d_gpost = norm_back(h_mid, g_post, d_y)
        d_hmid = d_hout + d_ymid
        d_hmid_b = d_hmid.astype(BF)
        d_hmid_b, early = lax.optimization_barrier((d_hmid_b, early))
        d_both = gather(jnp.concatenate([d_hout_b, d_hmid_b], axis=1))
        d_attn = dot_nt(d_hmid_b, w_o).astype(BF).reshape(q_rot.shape)
        d_attn2 = narrow(swap_tp(wide(d_attn)), unit)
        dobd, dobd2 = block_diag(d_attn), block_diag(d_attn2)

        dkv_q, dq_q, dgk_q = attn_bwd(lens_q, 4, Q_SIZES, kv_q, p_q, qbd[:n_q], dobd[:n_q], gk_row, cos_q, sin_q)
        dkv_d, dq_d, dgk_d = attn_bwd(len_d, 1, D_SIZES, kv_d, p_d, qbd[n_q:], dobd[n_q:], gk_row, cos_t, sin_t)
        d_qrot = jnp.concatenate([dq_q, dq_d], axis=0)[:, :q_rot.shape[1]].astype(BF)
        d_qrot, d_both = lax.optimization_barrier((d_qrot, d_both))
        d_qraw, d_gq = q_pull(d_qrot)
        d_xlast = psum_tp(dot_nt(d_qraw, w_q))
        d_qraw_all = gather(d_qraw)
        flat = lambda arr: arr.reshape(-1, arr.shape[-1])
        d_wkv = dot_tn(flat(x_q), flat(dkv_q)) + dot_tn(flat(x_d), flat(dkv_d))
        d_wkv, d_qraw_all = lax.optimization_barrier((d_wkv, d_qraw_all))
        d_wkv = lax.psum(d_wkv, 'dp')

        kv2_q, p2_q, _ = attn_fwd(x_q, order_q, lens_q, Q_MAX, 4, Q_SIZES, w_k2, w_v2, qbd2[:n_q], gk_row, cos_q, sin_q)
        kv2_d, p2_d, _ = attn_fwd(x_d, order_d, len_d, seq_len, 1, D_SIZES, w_k2, w_v2, qbd2[n_q:], gk_row, cos_t, sin_t)
        dkv2_q, _, _ = attn_bwd(lens_q, 4, Q_SIZES, kv2_q, p2_q, qbd2[:n_q], dobd2[:n_q], gk_row, cos_q, sin_q)
        dkv2_d, _, _ = attn_bwd(len_d, 1, D_SIZES, kv2_d, p2_d, qbd2[n_q:], dobd2[n_q:], gk_row, cos_t, sin_t)
        d_hid_q, dgin_q = attn_dx(hid_q, order_q, lens_q, Q_MAX, 4, Q_SIZES, dkv_q, dkv2_q, (w_k, w_v), (w_k2, w_v2), gin_row, d_xlast[:n_q], d_hmid[:n_q])
        d_hid_d, dgin_d = attn_dx(hid_d, order_d, len_d, seq_len, 1, D_SIZES, dkv_d, dkv2_d, (w_k, w_v), (w_k2, w_v2), gin_row, d_xlast[n_q:], d_hmid[n_q:])

        x_last_all, y_all, attn_all = early[:, :width], early[:, width:2 * width], early[:, 2 * width:]
        d_hout_all, d_hmid_all = d_both[:, :width], d_both[:, width:]
        act_all, act_all_pull = jax.vjp(swiglu, dot(y_all, w_gate).astype(BF).astype(F32), dot(y_all, w_up).astype(BF).astype(F32))
        d_gate_all, d_up_all = act_all_pull(dot_nt(d_hout_all, w_down).astype(BF).astype(F32))
        d_wdown = dot_tn(act_all.astype(BF), d_hout_all)
        d_wgate = dot_tn(y_all, d_gate_all.astype(BF))
        d_wup = dot_tn(y_all, d_up_all.astype(BF))
        d_wo = dot_tn(attn_all, d_hmid_all)
        d_wq = dot_tn(x_last_all, d_qraw_all)

        dp_sum = lambda vec: jnp.sum(lax.all_gather(vec, 'dp', axis=0), axis=0)
        d_heads = psum_tp(jnp.concatenate([d_gq, jnp.sum(dgk_q + dgk_d, axis=0)]))
        gains = dp_sum(jnp.concatenate([d_gpost, d_gfinal, d_heads]))
        d_gpost, d_gfinal, d_gq, d_gk = gains[:width], gains[width:2 * width], gains[2 * width:2 * width + HEAD], gains[2 * width + HEAD:]
        d_gin = dp_sum(jnp.sum(dgin_q + dgin_d, axis=0))
        return (loss_rows, d_hid_q, d_hid_d, d_wq, d_wkv[:, :kv_half], d_wkv[:, kv_half:], d_wo, d_wgate, d_wup, d_wdown,
                d_gin, d_gq, d_gk, d_gpost, d_gfinal)

    col_split = P(None, 'tp')
    row_split = P('tp', None)
    in_specs = (P('dp'), P('dp'), P('dp'), P('dp'), P('dp'), col_split, col_split, col_split, row_split, col_split, col_split, row_split, P(), P(), P(), P(), P())
    out_specs = (P('dp'), P('dp'), P('dp'), col_split, col_split, col_split, row_split, col_split, col_split, row_split, P(), P(), P(), P(), P())
    return jax.shard_map(device_step, mesh=mesh, in_specs=in_specs, out_specs=out_specs, check_vma=False)
```

```python
import functools
import jax
import jax.numpy as jnp
from jax import lax
from jax.experimental import pallas as pl
from jax.experimental.pallas import tpu as pltpu
from jax.sharding import PartitionSpec as P

NORM_EPS = 1e-6
ROPE_THETA = 1000000.0
TEMPERATURE = 0.05
HEAD = 128
Q_MAX = 128
BF = jnp.bfloat16
F32 = jnp.float32
SWAP = [(0, 1), (1, 0)]
VMEM = 60 * 1024 * 1024


def norm_rows(values, gain_vec):
    return values * lax.rsqrt(jnp.mean(values * values, axis=-1, keepdims=True) + NORM_EPS) * gain_vec


def norm_back(values, gain_vec, d_out):
    scale = lax.rsqrt(jnp.mean(values * values, axis=-1, keepdims=True) + NORM_EPS)
    g_dout = d_out * gain_vec
    d_values = scale * g_dout - values * scale ** 3 * jnp.mean(values * g_dout, axis=-1, keepdims=True)
    d_gain = jnp.sum((d_out * values * scale).reshape(-1, values.shape[-1]), axis=0)
    return d_values, d_gain


def rope_tables(positions):
    inv_freq = ROPE_THETA ** (-jnp.arange(0, HEAD, 2, dtype=F32) / HEAD)
    angles = positions.astype(F32)[:, None] * inv_freq
    cos_a, sin_a = jnp.cos(angles), jnp.sin(angles)
    return jnp.concatenate([cos_a, cos_a], axis=-1), jnp.concatenate([-sin_a, sin_a], axis=-1)


def rotate_query(q_raw, g_q, cos_t, sin_t):
    n_seq = q_raw.shape[0]
    normed = norm_rows(q_raw.reshape(n_seq, -1, HEAD).astype(F32), g_q)
    half = HEAD // 2
    swapped = jnp.concatenate([normed[..., half:], normed[..., :half]], axis=-1)
    return (normed * cos_t[:, None, :] + swapped * sin_t[:, None, :]).astype(BF)


def head_mask(n_rows, width):
    row_head = lax.rem(lax.broadcasted_iota(jnp.int32, (n_rows, width), 0), 16) // 2
    lane_head = lax.broadcasted_iota(jnp.int32, (n_rows, width), 1) // HEAD
    return row_head == lane_head


def block_diag(per_head):
    n_seq, n_q, _ = per_head.shape
    n_kv = n_q // 2
    wide = jnp.tile(per_head, (1, 1, n_kv))
    wide = jnp.where(head_mask(n_q, n_kv * HEAD)[None], wide, jnp.zeros_like(wide))
    return jnp.pad(wide, ((0, 0), (0, 16 - n_q), (0, 0)))


def take_diag(wide):
    kept = jnp.where(head_mask(wide.shape[0], wide.shape[1]), wide, 0.0)
    total = kept[:, :HEAD]
    for head in range(1, wide.shape[1] // HEAD):
        total = total + kept[:, head * HEAD:(head + 1) * HEAD]
    return total


def key_stats(k_raw):
    k_f = k_raw.astype(F32)
    scale = lax.rsqrt(jnp.mean(k_f * k_f, axis=-1, keepdims=True) + NORM_EPS)
    return k_f * scale, scale


def turn(values, cos_t, sin_t):
    return values * cos_t + pltpu.roll(values, HEAD // 2, 1) * sin_t


def variants(max_len, sizes, body):
    low = 0
    for size in sizes:
        pl.when(jnp.logical_and(max_len > low, max_len <= size))(functools.partial(body, size))
        low = size


NT = (((1,), (1,)), ((), ()))
TN = (((0,), (0,)), ((), ()))


def stacked(parts):
    return parts[0] if len(parts) == 1 else jnp.concatenate(parts, axis=0)


def row_lengths(lens_ref, first, group, shape):
    row_seq = lax.broadcasted_iota(jnp.int32, shape, 0) // 16
    lengths = jnp.full(shape, lens_ref[first], jnp.int32)
    for g in range(1, group):
        lengths = jnp.where(row_seq == g, lens_ref[first + g], lengths)
    return lengths


def fwd_body(do_norm, group, sizes, order_ref, lens_ref, *refs):
    h_refs, refs = refs[:group if do_norm else 1], refs[group if do_norm else 1:]
    if do_norm:
        gin_ref, wk_ref, wv_ref, qbd_ref, gk_ref, cos_ref, sin_ref, x_ref, kv_ref, p_ref, o_ref, rot_ref = refs
    else:
        wk_ref, wv_ref, qbd_ref, gk_ref, cos_ref, sin_ref, kv_ref, p_ref, o_ref, rot_ref = refs
        x_ref = h_refs[0]
    kv_half = wk_ref.shape[1]
    step = pl.program_id(0)

    def norm(size):
        chunk, model = 32, x_ref.shape[2]
        tiles = [slice(t, t + HEAD) for t in range(0, model, HEAD)]
        for g in range(group):
            def norm_chunk(c, carry, g=g):
                here = pl.ds(pl.multiple_of(c * chunk, chunk), chunk)
                squares = jnp.zeros((chunk, HEAD), F32)
                for t in tiles:
                    hid = h_refs[g][0, here, t].astype(F32)
                    squares = squares + hid * hid
                scale = lax.rsqrt(jnp.sum(squares, axis=-1, keepdims=True) / model + NORM_EPS)
                for t in tiles:
                    hid = h_refs[g][0, here, t].astype(F32)
                    x_ref[g, here, t] = (hid * scale * gin_ref[:, t]).astype(BF)
                return carry

            lax.fori_loop(0, size // chunk, norm_chunk, 0)
        if size < x_ref.shape[1]:
            x_ref[:, size:, :] = jnp.zeros((group, x_ref.shape[1] - size, model), BF)

    def run(size):
        if do_norm:
            norm(size)
        for at, w_ref in ((0, wk_ref), (kv_half, wv_ref)):
            x_val = x_ref[:, :size, :].reshape(group * size, x_ref.shape[2])
            out = jnp.dot(x_val, w_ref[...], preferred_element_type=F32)
            kv_ref[:, :size, at:at + kv_half] = out.astype(BF).reshape(group, size, kv_half)
        cos_t, sin_t = cos_ref[:size], sin_ref[:size]
        for g in range(group):
            for head in range(kv_half // HEAD):
                lanes = slice(head * HEAD, (head + 1) * HEAD)
                k_hat, _ = key_stats(kv_ref[g, :size, lanes])
                rot_ref[g, :size, lanes] = turn(k_hat * gk_ref[...], cos_t, sin_t).astype(BF)
        scores = stacked([lax.dot_general(qbd_ref[g], rot_ref[g, :size, :], NT, preferred_element_type=F32) for g in range(group)])
        valid = lax.broadcasted_iota(jnp.int32, scores.shape, 1) < row_lengths(lens_ref, step * group, group, scores.shape)
        scores = jnp.where(valid, scores * HEAD ** -0.5, -1e30)
        expd = jnp.exp(scores - jnp.max(scores, axis=-1, keepdims=True))
        prob = expd / jnp.sum(expd, axis=-1, keepdims=True)
        p_ref[:, :, :size] = prob.reshape(group, 16, size)
        prob = prob.astype(BF)
        mix = stacked([jnp.dot(prob[g * 16:(g + 1) * 16], kv_ref[g, :size, kv_half:], preferred_element_type=F32) for g in range(group)])
        o_ref[...] = take_diag(mix).reshape(group, 16, HEAD)

    variants(lens_ref[step * group + group - 1], sizes, run)


def attn_fwd(hid_or_x, order, lens, rows, group, sizes, w_k, w_v, qbd, g_k, cos_t, sin_t, g_in=None):
    n_seq, width = order.shape[0], 2 * w_k.shape[1]
    model = w_k.shape[0]
    do_norm = g_in is not None
    once = dict(pipeline_mode=pl.Buffered(buffer_count=1))
    by_group = lambda *shape: pl.BlockSpec((group,) + shape, lambda i, o, l: (i,) + (0,) * len(shape))
    whole = lambda arr: pl.BlockSpec(arr.shape, lambda i, o, l: (0,) * arr.ndim, **once)
    if do_norm:
        in_specs = [pl.BlockSpec((1, rows, model), lambda i, o, l, g=g: (o[i * group + g], 0, 0)) for g in range(group)]
        operands = [hid_or_x] * group + [g_in]
        in_specs.append(whole(g_in))
    else:
        in_specs, operands = [by_group(rows, model)], [hid_or_x]
    in_specs += [whole(w_k), whole(w_v), by_group(16, width // 2), whole(g_k), whole(cos_t), whole(sin_t)]
    operands += [w_k, w_v, qbd, g_k, cos_t, sin_t]
    out_specs = [by_group(rows, width), by_group(16, rows), by_group(16, HEAD), by_group(rows, width // 2)]
    out_shape = [jax.ShapeDtypeStruct((n_seq, rows, width), BF), jax.ShapeDtypeStruct((n_seq, 16, rows), F32), jax.ShapeDtypeStruct((n_seq, 16, HEAD), F32), jax.ShapeDtypeStruct((n_seq, rows, width // 2), BF)]
    if do_norm:
        out_specs.insert(0, by_group(rows, model))
        out_shape.insert(0, jax.ShapeDtypeStruct((n_seq, rows, model), BF))
    return pl.pallas_call(
        functools.partial(fwd_body, do_norm, group, sizes),
        grid_spec=pltpu.PrefetchScalarGridSpec(num_scalar_prefetch=2, grid=(n_seq // group,), in_specs=in_specs, out_specs=out_specs),
        out_shape=out_shape,
        compiler_params=pltpu.CompilerParams(dimension_semantics=("arbitrary",), vmem_limit_bytes=VMEM),
        cost_estimate=pl.CostEstimate(flops=2 * n_seq * rows * model * width, bytes_accessed=n_seq * rows * model * 4, transcendentals=0),
        name="attn_fwd" + ("_norm" if do_norm else "") + str(rows),
    )(order, lens, *operands)


def bwd_body(group, sizes, lens_ref, kv_ref, rot_ref, p_ref, qbd_ref, dobd_ref, gk_ref, cos_ref, sin_ref, dk_ref, dv_ref, dq_ref, dgk_ref, dkey_ref):
    step = pl.program_id(0)
    rows, width = kv_ref.shape[1], kv_ref.shape[2]
    kv_half = width // 2

    @pl.when(step == 0)
    def _():
        dgk_ref[...] = jnp.zeros_like(dgk_ref)

    def run(size):
        cos_t, sin_t = cos_ref[:size], sin_ref[:size]
        gk = gk_ref[...]
        prob = p_ref[:, :, :size].reshape(group * 16, size)
        d_prob = stacked([lax.dot_general(dobd_ref[g], kv_ref[g, :size, kv_half:], NT, preferred_element_type=F32) for g in range(group)])
        d_prob = d_prob.astype(BF).astype(F32)
        d_score = prob * (d_prob - jnp.sum(prob * d_prob, axis=-1, keepdims=True))
        d_score = (d_score * HEAD ** -0.5).astype(BF)
        prob = prob.astype(BF)
        for g in range(group):
            d_key = lax.dot_general(d_score[g * 16:(g + 1) * 16], qbd_ref[g], TN, preferred_element_type=F32)
            dkey_ref[g, :size, :] = d_key.astype(BF)
            d_val = lax.dot_general(prob[g * 16:(g + 1) * 16], dobd_ref[g], TN, preferred_element_type=F32)
            dv_ref[g, :size, :] = d_val.astype(BF)
        d_gain = jnp.zeros((8, HEAD), F32)
        for g in range(group):
            for head in range(kv_half // HEAD):
                lanes = slice(head * HEAD, (head + 1) * HEAD)
                k_hat, scale = key_stats(kv_ref[g, :size, lanes])
                d_norm = turn(dkey_ref[g, :size, lanes].astype(F32), cos_t, -sin_t)
                d_gain = d_gain + jnp.sum((d_norm * k_hat).reshape(size // 8, 8, HEAD), axis=0)
                d_hat = d_norm * gk
                d_raw = scale * (d_hat - k_hat * jnp.mean(k_hat * d_hat, axis=-1, keepdims=True))
                dk_ref[g, :size, lanes] = d_raw.astype(BF)
        dgk_ref[...] += d_gain
        d_query = stacked([jnp.dot(d_score[g * 16:(g + 1) * 16], rot_ref[g, :size, :], preferred_element_type=F32) for g in range(group)])
        dq_ref[...] = take_diag(d_query).reshape(group, 16, HEAD)
        if size < rows:
            dk_ref[:, size:, :] = jnp.zeros((group, rows - size, kv_half), BF)
            dv_ref[:, size:, :] = jnp.zeros((group, rows - size, kv_half), BF)

    variants(lens_ref[step * group + group - 1], sizes, run)


def attn_bwd(lens, group, sizes, kv, rot, prob, qbd, dobd, g_k, cos_t, sin_t):
    n_seq, rows, width = kv.shape
    once = dict(pipeline_mode=pl.Buffered(buffer_count=1))
    by_group = lambda *shape: pl.BlockSpec((group,) + shape, lambda i, l: (i,) + (0,) * len(shape))
    whole = lambda arr: pl.BlockSpec(arr.shape, lambda i, l: (0,) * arr.ndim, **once)
    return pl.pallas_call(
        functools.partial(bwd_body, group, sizes),
        grid_spec=pltpu.PrefetchScalarGridSpec(
            num_scalar_prefetch=1, grid=(n_seq // group,),
            in_specs=[by_group(rows, width), by_group(rows, width // 2), by_group(16, rows), by_group(16, width // 2), by_group(16, width // 2), whole(g_k), whole(cos_t), whole(sin_t)],
            out_specs=[by_group(rows, width // 2), by_group(rows, width // 2), by_group(16, HEAD), pl.BlockSpec((8, HEAD), lambda i, l: (0, 0))],
            scratch_shapes=[pltpu.VMEM((group, rows, width // 2), BF)]),
        out_shape=[jax.ShapeDtypeStruct((n_seq, rows, width // 2), BF)] * 2 + [jax.ShapeDtypeStruct((n_seq, 16, HEAD), F32), jax.ShapeDtypeStruct((8, HEAD), F32)],
        compiler_params=pltpu.CompilerParams(dimension_semantics=("arbitrary",), vmem_limit_bytes=VMEM),
        cost_estimate=pl.CostEstimate(flops=20 * 1000 * n_seq * rows * width // 8, bytes_accessed=n_seq * rows * width * 4, transcendentals=0),
        name="attn_bwd" + str(rows),
    )(lens, kv, rot, prob, qbd, dobd, g_k, cos_t, sin_t)


def dx_body(group, n_seq, sizes, order_ref, lens_ref, dk_ref, dv_ref, dk2_ref, dv2_ref, wk_ref, wv_ref, wk2_ref, wv2_ref, h_ref, gin_ref, dxl_ref, dhm_ref, out_ref, dgin_ref, dx_ref):
    step = pl.program_id(0)
    rows, model = h_ref.shape[1], h_ref.shape[2]
    kv_half = dk_ref.shape[2]
    inner = lax.rem(step, group)
    turn_in = lax.rem(step // group, 2)
    part_cols = model // group
    wide_cols = min(part_cols, 512)

    @pl.when(step == 0)
    def _():
        dgin_ref[...] = jnp.zeros_like(dgin_ref)

    def multiply(k_ref, v_ref, key_w, val_w, add, size):
        for j in range(part_cols // wide_cols):
            cols = pl.ds(pl.multiple_of(inner * part_cols + j * wide_cols, wide_cols), wide_cols)
            d_keys = k_ref[:, :size, :].reshape(group * size, kv_half)
            d_vals = v_ref[:, :size, :].reshape(group * size, kv_half)
            part = lax.dot_general(d_keys, key_w[cols, :], NT, preferred_element_type=F32)
            part = part + lax.dot_general(d_vals, val_w[cols, :], NT, preferred_element_type=F32)
            part = part.reshape(group, size, wide_cols)
            dx_ref[turn_in, :, :size, cols] = dx_ref[turn_in, :, :size, cols] + part if add else part

    def finish(size):
        slot = 1 - turn_in
        last = lens_ref[step - group] - 1
        dx_ref[slot, inner, pl.ds(last, 1), :] += dxl_ref[0]
        chunk = 32
        tiles = [slice(t, t + HEAD) for t in range(0, model, HEAD)]

        def finish_chunk(c, carry):
            start = pl.multiple_of(c * chunk, chunk)
            here = pl.ds(start, chunk)
            at_last = lax.broadcasted_iota(jnp.int32, (chunk, HEAD), 0) + start == last
            squares, cross = jnp.zeros((chunk, HEAD), F32), jnp.zeros((chunk, HEAD), F32)
            for t in tiles:
                hid = h_ref[0, here, t].astype(F32)
                squares = squares + hid * hid
                cross = cross + hid * (dx_ref[slot, inner, here, t] * gin_ref[:, t])
            scale = lax.rsqrt(jnp.sum(squares, axis=-1, keepdims=True) / model + NORM_EPS)
            slope = scale * scale * scale * (jnp.sum(cross, axis=-1, keepdims=True) / model)
            for t in tiles:
                hid = h_ref[0, here, t].astype(F32)
                d_x = dx_ref[slot, inner, here, t] * scale
                dgin_ref[:, t] += jnp.sum((d_x * hid).reshape(chunk // 8, 8, HEAD), axis=0)
                d_hid = d_x * gin_ref[:, t] - hid * slope
                out_ref[0, here, t] = (d_hid + jnp.where(at_last, dhm_ref[0][:, t], 0.0)).astype(BF)
            return carry

        lax.fori_loop(0, size // chunk, finish_chunk, 0)
        if size < out_ref.shape[1]:
            out_ref[0, size:, :] = jnp.zeros((out_ref.shape[1] - size, model), BF)

    first = step - inner
    longest = jnp.where(step < n_seq, lens_ref[jnp.minimum(first, n_seq - group) + group - 1], 0)
    variants(longest, sizes, functools.partial(multiply, dk_ref, dv_ref, wk_ref, wv_ref, False))
    variants(longest, sizes, functools.partial(multiply, dk2_ref, dv2_ref, wk2_ref, wv2_ref, True))
    pl.when(step >= group)(lambda: variants(lens_ref[jnp.maximum(first - group, 0) + group - 1], sizes, finish))


def attn_dx(hid, order, lens, rows, group, sizes, d_own, d_oth, w_own, w_oth, g_in, d_xlast, d_hmid):
    n_seq, seq_len, model = hid.shape
    width = 2 * w_own[0].shape[1]
    weights = tuple(w_own) + tuple(w_oth)
    once = dict(pipeline_mode=pl.Buffered(buffer_count=1))
    of_group = pl.BlockSpec((group, rows, width // 2), lambda i, o, l: (jnp.minimum(i // group, n_seq // group - 1), 0, 0))
    whole = lambda arr: pl.BlockSpec(arr.shape, lambda i, o, l: (0,) * arr.ndim, **once)
    late = lambda i: jnp.maximum(i - group, 0)
    one_row = pl.BlockSpec((1, 1, model), lambda i, o, l: (late(i), 0, 0))
    return pl.pallas_call(
        functools.partial(dx_body, group, n_seq, sizes),
        grid_spec=pltpu.PrefetchScalarGridSpec(
            num_scalar_prefetch=2, grid=(n_seq + group,),
            in_specs=[of_group] * 4 + [whole(w) for w in weights] + [pl.BlockSpec((1, rows, model), lambda i, o, l: (o[late(i)], 0, 0)),
                      whole(g_in), one_row, one_row],
            out_specs=[pl.BlockSpec((1, seq_len, model), lambda i, o, l: (o[late(i)], 0, 0)), pl.BlockSpec((8, model), lambda i, o, l: (0, 0))],
            scratch_shapes=[pltpu.VMEM((2, group, rows, model), F32)]),
        out_shape=[jax.ShapeDtypeStruct(hid.shape, BF), jax.ShapeDtypeStruct((8, model), F32)],
        compiler_params=pltpu.CompilerParams(dimension_semantics=("arbitrary",), vmem_limit_bytes=VMEM),
        cost_estimate=pl.CostEstimate(flops=4 * n_seq * rows * model * width, bytes_accessed=hid.size * 4, transcendentals=0),
        name="attn_dx" + str(rows),
    )(order, lens, *d_own, *d_oth, *weights, hid, g_in, d_xlast[:, None, :], d_hmid[:, None, :])


def wide(values):
    return values.astype(F32)


def narrow(values, unit):
    return (values * unit).astype(BF)


def swap_tp(values):
    return lax.ppermute(values, 'tp', SWAP)


def psum_tp(values):
    return values + swap_tp(values)


def swiglu(gate_in, up_in):
    return jax.nn.silu(gate_in) * up_in


def final_head(h_out, g_final):
    z_norm = norm_rows(h_out, g_final)
    return z_norm * lax.rsqrt(jnp.sum(z_norm * z_norm, axis=-1, keepdims=True))


def dot(a, b):
    return jnp.dot(a, b, preferred_element_type=F32)


def dot_nt(a, b):
    return lax.dot_general(a, b, NT, preferred_element_type=F32)


def dot_tn(a, b):
    return lax.dot_general(a, b, TN, preferred_element_type=F32)


Q_SIZES = (32, 64, 96, 128)
D_SIZES = (128, 256, 384, 512)


def solution(mesh):
    dp_size = mesh.shape['dp']

    def device_step(hid_q, hid_d, len_q, len_d, pos_doc, w_q, w_k, w_v, w_o, w_gate, w_up, w_down, g_in, g_q, g_k, g_post, g_final):
        g_in, g_q, g_k, g_post, g_final = (gain.astype(F32) for gain in (g_in, g_q, g_k, g_post, g_final))
        n_q, n_d = hid_q.shape[0], hid_d.shape[0]
        seq_len = hid_q.shape[1]
        n_query = n_q * dp_size

        ids = jnp.arange(n_q)
        before = (len_q[None, :] < len_q[:, None]) | ((len_q[None, :] == len_q[:, None]) & (ids[None, :] < ids[:, None]))
        rank = jnp.sum(before, axis=1)
        is_rank = rank[None, :] == ids[:, None]
        order_q = jnp.sum(jnp.where(is_rank, ids[None, :], 0), axis=1).astype(jnp.int32)
        lens_q = jnp.sum(jnp.where(is_rank, len_q[None, :], 0), axis=1).astype(jnp.int32)
        pos_sorted = jnp.sum(jnp.where(is_rank, pos_doc[None, :], 0), axis=1).astype(jnp.int32)
        order_d = jnp.arange(n_d, dtype=jnp.int32)
        lens = jnp.concatenate([lens_q, len_d])
        unit = jnp.minimum(len_d[0], 1).astype(F32)

        kv_half = w_k.shape[1]
        slab_rows = w_k.shape[0] // dp_size
        my_slab = lambda arr: lax.dynamic_slice_in_dim(arr, lax.axis_index('dp') * slab_rows, slab_rows, axis=0)
        slab = jnp.concatenate([my_slab(w_k), my_slab(w_v)], axis=1)
        slab2 = swap_tp(wide(slab))

        h_last = jnp.concatenate([hid_q[order_q, lens_q - 1], hid_d[order_d, len_d - 1]], axis=0).astype(F32)
        x_last = norm_rows(h_last, g_in).astype(BF)
        q_raw = dot(x_last, w_q).astype(BF)
        q_cos, q_sin = rope_tables(lens - 1)
        q_rot, q_pull = jax.vjp(lambda raw, gain: rotate_query(raw, gain, q_cos, q_sin), q_raw, g_q)
        q_rot2 = narrow(swap_tp(wide(q_rot)), unit)
        qbd, qbd2 = block_diag(q_rot), block_diag(q_rot2)

        cos_t, sin_t = rope_tables(jnp.arange(seq_len))
        cos_q, sin_q = cos_t[:Q_MAX], sin_t[:Q_MAX]
        gin_row, gk_row = g_in[None, :], g_k[None, :]
        x_d, kv_d, p_d, o_d, rot_d = attn_fwd(hid_d, order_d, len_d, seq_len, 1, D_SIZES, w_k, w_v, qbd[n_q:], gk_row, cos_t, sin_t, gin_row)
        slab2, x_d = lax.optimization_barrier((slab2, x_d))
        w_kv2 = lax.all_gather(slab2, 'dp', axis=0, tiled=True)
        x_q, kv_q, p_q, o_q, rot_q = attn_fwd(hid_q, order_q, lens_q, Q_MAX, 4, Q_SIZES, w_k, w_v, qbd[:n_q], gk_row, cos_q, sin_q, gin_row)
        attn_out = jnp.concatenate([o_q, o_d], axis=0)[:, :q_rot.shape[1]].astype(BF).reshape(n_q + n_d, -1)

        h_mid = h_last + psum_tp(dot(attn_out, w_o))
        y_norm = norm_rows(h_mid, g_post).astype(BF)
        width = h_last.shape[1]
        pad_rows = -(n_q + n_d) % 8
        gather = lambda arr: narrow(lax.all_gather(wide(jnp.pad(arr, ((0, pad_rows), (0, 0)))), 'dp', axis=0, tiled=True), unit)
        y_norm, w_kv2 = lax.optimization_barrier((y_norm, w_kv2))
        w_kv2 = narrow(w_kv2, unit)
        w_k2, w_v2 = w_kv2[:, :kv_half], w_kv2[:, kv_half:]
        gate_val = dot(y_norm, w_gate).astype(BF)
        up_val = dot(y_norm, w_up).astype(BF)
        hidden_act, act_pull = jax.vjp(swiglu, gate_val.astype(F32), up_val.astype(F32))
        hidden_act = hidden_act.astype(BF)
        early = gather(jnp.concatenate([x_last, y_norm, attn_out, hidden_act], axis=1))
        h_out = h_mid + psum_tp(dot(hidden_act, w_down))
        emb, head_pull = jax.vjp(final_head, h_out, g_final)
        emb_q, emb_d = emb[:n_q], emb[n_q:]

        all_docs = lax.all_gather(emb_d, 'dp', axis=0, tiled=True)
        logits = jnp.einsum('qd,kd->qk', emb_q, all_docs, precision=lax.Precision.HIGHEST) / TEMPERATURE
        log_norm = jax.nn.logsumexp(logits, axis=1)
        is_pos = jnp.arange(all_docs.shape[0])[None, :] == pos_sorted[:, None]
        loss_sorted = log_norm - jnp.sum(jnp.where(is_pos, logits, 0.0), axis=1)
        loss_rows = jnp.sum(jnp.where(is_rank, loss_sorted[:, None], 0.0), axis=0)
        d_logits = (jnp.exp(logits - log_norm[:, None]) - is_pos.astype(F32)) / (n_query * TEMPERATURE)
        d_emb_q = jnp.einsum('qk,kd->qd', d_logits, all_docs, precision=lax.Precision.HIGHEST)
        d_docs = jnp.einsum('qk,qd->kd', d_logits, emb_q, precision=lax.Precision.HIGHEST)
        d_docs = lax.all_to_all(d_docs, 'dp', 0, 0, tiled=True)
        d_emb_d = jnp.sum(d_docs.reshape(dp_size, n_d, width), axis=0)

        d_hout, d_gfinal = head_pull(jnp.concatenate([d_emb_q, d_emb_d], axis=0))
        d_hout_b = d_hout.astype(BF)
        d_act = dot_nt(d_hout_b, w_down).astype(BF)
        d_gate, d_up = (d_in.astype(BF) for d_in in act_pull(d_act.astype(F32)))
        d_y = psum_tp(dot_nt(d_gate, w_gate) + dot_nt(d_up, w_up))
        d_ymid, d_gpost = norm_back(h_mid, g_post, d_y)
        d_hmid = d_hout + d_ymid
        d_hmid_b = d_hmid.astype(BF)
        d_hmid_b, early = lax.optimization_barrier((d_hmid_b, early))
        d_both = gather(jnp.concatenate([d_hout_b, d_hmid_b, d_gate, d_up], axis=1))
        d_attn = dot_nt(d_hmid_b, w_o).astype(BF).reshape(q_rot.shape)
        d_attn2 = narrow(swap_tp(wide(d_attn)), unit)
        dobd, dobd2 = block_diag(d_attn), block_diag(d_attn2)

        dk_q, dv_q, dq_q, dgk_q = attn_bwd(lens_q, 4, Q_SIZES, kv_q, rot_q, p_q, qbd[:n_q], dobd[:n_q], gk_row, cos_q, sin_q)
        dk_d, dv_d, dq_d, dgk_d = attn_bwd(len_d, 1, D_SIZES, kv_d, rot_d, p_d, qbd[n_q:], dobd[n_q:], gk_row, cos_t, sin_t)
        d_qrot = jnp.concatenate([dq_q, dq_d], axis=0)[:, :q_rot.shape[1]].astype(BF)
        d_qraw, d_gq = q_pull(d_qrot)
        d_xlast = psum_tp(dot_nt(d_qraw, w_q))
        flat = lambda arr: arr.reshape(-1, arr.shape[-1])
        d_wk = dot_tn(flat(x_q), flat(dk_q)) + dot_tn(flat(x_d), flat(dk_d))
        d_wv = dot_tn(flat(x_q), flat(dv_q)) + dot_tn(flat(x_d), flat(dv_d))
        d_wk, d_wv, d_both = lax.optimization_barrier((d_wk, d_wv, d_both))
        d_wk, d_wv = lax.psum((d_wk, d_wv), 'dp')

        kv2_q, p2_q, _, rot2_q = attn_fwd(x_q, order_q, lens_q, Q_MAX, 4, Q_SIZES, w_k2, w_v2, qbd2[:n_q], gk_row, cos_q, sin_q)
        kv2_d, p2_d, _, rot2_d = attn_fwd(x_d, order_d, len_d, seq_len, 1, D_SIZES, w_k2, w_v2, qbd2[n_q:], gk_row, cos_t, sin_t)
        dk2_q, dv2_q, _, _ = attn_bwd(lens_q, 4, Q_SIZES, kv2_q, rot2_q, p2_q, qbd2[:n_q], dobd2[:n_q], gk_row, cos_q, sin_q)
        dk2_d, dv2_d, _, _ = attn_bwd(len_d, 1, D_SIZES, kv2_d, rot2_d, p2_d, qbd2[n_q:], dobd2[n_q:], gk_row, cos_t, sin_t)
        d_hid_q, dgin_q = attn_dx(hid_q, order_q, lens_q, Q_MAX, 4, Q_SIZES, (dk_q, dv_q), (dk2_q, dv2_q), (w_k, w_v), (w_k2, w_v2), gin_row, d_xlast[:n_q], d_hmid[:n_q])
        d_hid_d, dgin_d = attn_dx(hid_d, order_d, len_d, seq_len, 1, D_SIZES, (dk_d, dv_d), (dk2_d, dv2_d), (w_k, w_v), (w_k2, w_v2), gin_row, d_xlast[n_q:], d_hmid[n_q:])

        d_qraw, d_wk, d_wv, dgin_q = lax.optimization_barrier((d_qraw, d_wk, d_wv, dgin_q))
        d_qraw_all = gather(d_qraw)
        kv_width = attn_out.shape[1]
        x_last_all, y_all = early[:, :width], early[:, width:2 * width]
        attn_all, act_all = early[:, 2 * width:2 * width + kv_width], early[:, 2 * width + kv_width:]
        d_hout_all, d_hmid_all = d_both[:, :width], d_both[:, width:2 * width]
        d_gate_all, d_up_all = jnp.split(d_both[:, 2 * width:], 2, axis=1)
        d_wdown = dot_tn(act_all, d_hout_all)
        d_wgate = dot_tn(y_all, d_gate_all)
        d_wup = dot_tn(y_all, d_up_all)
        d_wo = dot_tn(attn_all, d_hmid_all)
        d_wq = dot_tn(x_last_all, d_qraw_all)

        dp_sum = lambda vec: jnp.sum(lax.all_gather(vec, 'dp', axis=0), axis=0)
        d_heads = psum_tp(jnp.concatenate([d_gq, jnp.sum(dgk_q + dgk_d, axis=0)]))
        gains = dp_sum(jnp.concatenate([d_gpost, d_gfinal, jnp.sum(dgin_q + dgin_d, axis=0), d_heads]))
        d_gpost, d_gfinal, d_gin, d_heads = jnp.split(gains, (width, 2 * width, 3 * width))
        d_gq, d_gk = d_heads[:HEAD], d_heads[HEAD:]
        return (loss_rows, d_hid_q, d_hid_d, d_wq, d_wk, d_wv, d_wo, d_wgate, d_wup, d_wdown,
                d_gin, d_gq, d_gk, d_gpost, d_gfinal)

    col_split = P(None, 'tp')
    row_split = P('tp', None)
    in_specs = (P('dp'), P('dp'), P('dp'), P('dp'), P('dp'), col_split, col_split, col_split, row_split, col_split, col_split, row_split, P(), P(), P(), P(), P())
    out_specs = (P('dp'), P('dp'), P('dp'), col_split, col_split, col_split, row_split, col_split, col_split, row_split, P(), P(), P(), P(), P())
    return jax.shard_map(device_step, mesh=mesh, in_specs=in_specs, out_specs=out_specs, check_vma=False)
```

```python
import functools
import jax
import jax.numpy as jnp
from jax import lax
from jax.experimental import pallas as pl
from jax.experimental.pallas import tpu as pltpu
from jax.sharding import PartitionSpec as P

NORM_EPS = 1e-6
ROPE_THETA = 1000000.0
TEMPERATURE = 0.05
HEAD = 128
Q_MAX = 128
BF = jnp.bfloat16
F32 = jnp.float32
SWAP = [(0, 1), (1, 0)]
VMEM = 60 * 1024 * 1024


def norm_rows(values, gain_vec):
    return values * lax.rsqrt(jnp.mean(values * values, axis=-1, keepdims=True) + NORM_EPS) * gain_vec


def norm_back(values, gain_vec, d_out):
    scale = lax.rsqrt(jnp.mean(values * values, axis=-1, keepdims=True) + NORM_EPS)
    g_dout = d_out * gain_vec
    d_values = scale * g_dout - values * scale ** 3 * jnp.mean(values * g_dout, axis=-1, keepdims=True)
    d_gain = jnp.sum((d_out * values * scale).reshape(-1, values.shape[-1]), axis=0)
    return d_values, d_gain


def rope_tables(positions):
    inv_freq = ROPE_THETA ** (-jnp.arange(0, HEAD, 2, dtype=F32) / HEAD)
    angles = positions.astype(F32)[:, None] * inv_freq
    cos_a, sin_a = jnp.cos(angles), jnp.sin(angles)
    return jnp.concatenate([cos_a, cos_a], axis=-1), jnp.concatenate([-sin_a, sin_a], axis=-1)


def rotate_query(q_raw, g_q, cos_t, sin_t):
    n_seq = q_raw.shape[0]
    normed = norm_rows(q_raw.reshape(n_seq, -1, HEAD).astype(F32), g_q)
    half = HEAD // 2
    swapped = jnp.concatenate([normed[..., half:], normed[..., :half]], axis=-1)
    return (normed * cos_t[:, None, :] + swapped * sin_t[:, None, :]).astype(BF)


def head_mask(n_rows, width):
    row_head = lax.rem(lax.broadcasted_iota(jnp.int32, (n_rows, width), 0), 16) // 2
    lane_head = lax.broadcasted_iota(jnp.int32, (n_rows, width), 1) // HEAD
    return row_head == lane_head


def block_diag(per_head):
    n_seq, n_q, _ = per_head.shape
    n_kv = n_q // 2
    wide = jnp.tile(per_head, (1, 1, n_kv))
    wide = jnp.where(head_mask(n_q, n_kv * HEAD)[None], wide, jnp.zeros_like(wide))
    return jnp.pad(wide, ((0, 0), (0, 16 - n_q), (0, 0)))


def take_diag(wide):
    kept = jnp.where(head_mask(wide.shape[0], wide.shape[1]), wide, 0.0)
    total = kept[:, :HEAD]
    for head in range(1, wide.shape[1] // HEAD):
        total = total + kept[:, head * HEAD:(head + 1) * HEAD]
    return total


def key_stats(k_raw):
    k_f = k_raw.astype(F32)
    scale = lax.rsqrt(jnp.mean(k_f * k_f, axis=-1, keepdims=True) + NORM_EPS)
    return k_f * scale, scale


def turn(values, cos_t, sin_t):
    return values * cos_t + pltpu.roll(values, HEAD // 2, 1) * sin_t


def variants(max_len, sizes, body):
    low = 0
    for size in sizes:
        pl.when(jnp.logical_and(max_len > low, max_len <= size))(functools.partial(body, size))
        low = size


NT = (((1,), (1,)), ((), ()))
TN = (((0,), (0,)), ((), ()))


def stacked(parts):
    return parts[0] if len(parts) == 1 else jnp.concatenate(parts, axis=0)


def row_lengths(lens_ref, first, group, shape):
    row_seq = lax.broadcasted_iota(jnp.int32, shape, 0) // 16
    lengths = jnp.full(shape, lens_ref[first], jnp.int32)
    for g in range(1, group):
        lengths = jnp.where(row_seq == g, lens_ref[first + g], lengths)
    return lengths


def fwd_body(do_norm, group, sizes, order_ref, lens_ref, *refs):
    h_refs, refs = refs[:group if do_norm else 1], refs[group if do_norm else 1:]
    if do_norm:
        gin_ref, wk_ref, wv_ref, qbd_ref, gk_ref, cos_ref, sin_ref, x_ref, kv_ref, p_ref, o_ref, rot_ref = refs
    else:
        wk_ref, wv_ref, qbd_ref, gk_ref, cos_ref, sin_ref, kv_ref, p_ref, o_ref, rot_ref = refs
        x_ref = h_refs[0]
    kv_half = wk_ref.shape[1]
    step = pl.program_id(0)

    def norm(size):
        chunk, model = 32, x_ref.shape[2]
        tiles = [slice(t, t + HEAD) for t in range(0, model, HEAD)]
        for g in range(group):
            def norm_chunk(c, carry, g=g):
                here = pl.ds(pl.multiple_of(c * chunk, chunk), chunk)
                squares = jnp.zeros((chunk, HEAD), F32)
                for t in tiles:
                    hid = h_refs[g][0, here, t].astype(F32)
                    squares = squares + hid * hid
                scale = lax.rsqrt(jnp.sum(squares, axis=-1, keepdims=True) / model + NORM_EPS)
                for t in tiles:
                    hid = h_refs[g][0, here, t].astype(F32)
                    x_ref[g, here, t] = (hid * scale * gin_ref[:, t]).astype(BF)
                return carry

            lax.fori_loop(0, size // chunk, norm_chunk, 0)
        if size < x_ref.shape[1]:
            x_ref[:, size:, :] = jnp.zeros((group, x_ref.shape[1] - size, model), BF)

    def run(size):
        if do_norm:
            norm(size)
        for at, w_ref in ((0, wk_ref), (kv_half, wv_ref)):
            x_val = x_ref[:, :size, :].reshape(group * size, x_ref.shape[2])
            out = jnp.dot(x_val, w_ref[...], preferred_element_type=F32)
            kv_ref[:, :size, at:at + kv_half] = out.astype(BF).reshape(group, size, kv_half)
        cos_t, sin_t = cos_ref[:size], sin_ref[:size]
        for g in range(group):
            for head in range(kv_half // HEAD):
                lanes = slice(head * HEAD, (head + 1) * HEAD)
                k_hat, _ = key_stats(kv_ref[g, :size, lanes])
                rot_ref[g, :size, lanes] = turn(k_hat * gk_ref[...], cos_t, sin_t).astype(BF)
        scores = stacked([lax.dot_general(qbd_ref[g], rot_ref[g, :size, :], NT, preferred_element_type=F32) for g in range(group)])
        valid = lax.broadcasted_iota(jnp.int32, scores.shape, 1) < row_lengths(lens_ref, step * group, group, scores.shape)
        scores = jnp.where(valid, scores * HEAD ** -0.5, -1e30)
        expd = jnp.exp(scores - jnp.max(scores, axis=-1, keepdims=True))
        prob = expd / jnp.sum(expd, axis=-1, keepdims=True)
        p_ref[:, :, :size] = prob.reshape(group, 16, size)
        prob = prob.astype(BF)
        mix = stacked([jnp.dot(prob[g * 16:(g + 1) * 16], kv_ref[g, :size, kv_half:], preferred_element_type=F32) for g in range(group)])
        o_ref[...] = take_diag(mix).reshape(group, 16, HEAD)

    variants(lens_ref[step * group + group - 1], sizes, run)


def attn_fwd(hid_or_x, order, lens, rows, group, sizes, w_k, w_v, qbd, g_k, cos_t, sin_t, g_in=None):
    n_seq, width = order.shape[0], 2 * w_k.shape[1]
    model = w_k.shape[0]
    do_norm = g_in is not None
    once = dict(pipeline_mode=pl.Buffered(buffer_count=1))
    by_group = lambda *shape: pl.BlockSpec((group,) + shape, lambda i, o, l: (i,) + (0,) * len(shape))
    whole = lambda arr: pl.BlockSpec(arr.shape, lambda i, o, l: (0,) * arr.ndim, **once)
    if do_norm:
        in_specs = [pl.BlockSpec((1, rows, model), lambda i, o, l, g=g: (o[i * group + g], 0, 0)) for g in range(group)]
        operands = [hid_or_x] * group + [g_in]
        in_specs.append(whole(g_in))
    else:
        in_specs, operands = [by_group(rows, model)], [hid_or_x]
    in_specs += [whole(w_k), whole(w_v), by_group(16, width // 2), whole(g_k), whole(cos_t), whole(sin_t)]
    operands += [w_k, w_v, qbd, g_k, cos_t, sin_t]
    out_specs = [by_group(rows, width), by_group(16, rows), by_group(16, HEAD), by_group(rows, width // 2)]
    out_shape = [jax.ShapeDtypeStruct((n_seq, rows, width), BF), jax.ShapeDtypeStruct((n_seq, 16, rows), F32), jax.ShapeDtypeStruct((n_seq, 16, HEAD), F32), jax.ShapeDtypeStruct((n_seq, rows, width // 2), BF)]
    if do_norm:
        out_specs.insert(0, by_group(rows, model))
        out_shape.insert(0, jax.ShapeDtypeStruct((n_seq, rows, model), BF))
    return pl.pallas_call(
        functools.partial(fwd_body, do_norm, group, sizes),
        grid_spec=pltpu.PrefetchScalarGridSpec(num_scalar_prefetch=2, grid=(n_seq // group,), in_specs=in_specs, out_specs=out_specs),
        out_shape=out_shape,
        compiler_params=pltpu.CompilerParams(dimension_semantics=("arbitrary",), vmem_limit_bytes=VMEM),
        cost_estimate=pl.CostEstimate(flops=2 * n_seq * rows * model * width, bytes_accessed=n_seq * rows * model * 4, transcendentals=0),
        name="attn_fwd" + ("_norm" if do_norm else "") + str(rows),
    )(order, lens, *operands)


def bwd_body(group, sizes, lens_ref, kv_ref, rot_ref, p_ref, qbd_ref, dobd_ref, gk_ref, cos_ref, sin_ref, dk_ref, dv_ref, dq_ref, dgk_ref, dkey_ref):
    step = pl.program_id(0)
    rows, width = kv_ref.shape[1], kv_ref.shape[2]
    kv_half = width // 2

    @pl.when(step == 0)
    def _():
        dgk_ref[...] = jnp.zeros_like(dgk_ref)

    def run(size):
        cos_t, sin_t = cos_ref[:size], sin_ref[:size]
        gk = gk_ref[...]
        prob = p_ref[:, :, :size].reshape(group * 16, size)
        d_prob = stacked([lax.dot_general(dobd_ref[g], kv_ref[g, :size, kv_half:], NT, preferred_element_type=F32) for g in range(group)])
        d_prob = d_prob.astype(BF).astype(F32)
        d_score = prob * (d_prob - jnp.sum(prob * d_prob, axis=-1, keepdims=True))
        d_score = (d_score * HEAD ** -0.5).astype(BF)
        prob = prob.astype(BF)
        for g in range(group):
            d_key = lax.dot_general(d_score[g * 16:(g + 1) * 16], qbd_ref[g], TN, preferred_element_type=F32)
            dkey_ref[g, :size, :] = d_key.astype(BF)
            d_val = lax.dot_general(prob[g * 16:(g + 1) * 16], dobd_ref[g], TN, preferred_element_type=F32)
            dv_ref[g, :size, :] = d_val.astype(BF)
        d_gain = jnp.zeros((8, HEAD), F32)
        for g in range(group):
            for head in range(kv_half // HEAD):
                lanes = slice(head * HEAD, (head + 1) * HEAD)
                k_hat, scale = key_stats(kv_ref[g, :size, lanes])
                d_norm = turn(dkey_ref[g, :size, lanes].astype(F32), cos_t, -sin_t)
                d_gain = d_gain + jnp.sum((d_norm * k_hat).reshape(size // 8, 8, HEAD), axis=0)
                d_hat = d_norm * gk
                d_raw = scale * (d_hat - k_hat * jnp.mean(k_hat * d_hat, axis=-1, keepdims=True))
                dk_ref[g, :size, lanes] = d_raw.astype(BF)
        dgk_ref[...] += d_gain
        d_query = stacked([jnp.dot(d_score[g * 16:(g + 1) * 16], rot_ref[g, :size, :], preferred_element_type=F32) for g in range(group)])
        dq_ref[...] = take_diag(d_query).reshape(group, 16, HEAD)
        if size < rows:
            dk_ref[:, size:, :] = jnp.zeros((group, rows - size, kv_half), BF)
            dv_ref[:, size:, :] = jnp.zeros((group, rows - size, kv_half), BF)

    variants(lens_ref[step * group + group - 1], sizes, run)


def attn_bwd(lens, group, sizes, kv, rot, prob, qbd, dobd, g_k, cos_t, sin_t):
    n_seq, rows, width = kv.shape
    once = dict(pipeline_mode=pl.Buffered(buffer_count=1))
    by_group = lambda *shape: pl.BlockSpec((group,) + shape, lambda i, l: (i,) + (0,) * len(shape))
    whole = lambda arr: pl.BlockSpec(arr.shape, lambda i, l: (0,) * arr.ndim, **once)
    return pl.pallas_call(
        functools.partial(bwd_body, group, sizes),
        grid_spec=pltpu.PrefetchScalarGridSpec(
            num_scalar_prefetch=1, grid=(n_seq // group,),
            in_specs=[by_group(rows, width), by_group(rows, width // 2), by_group(16, rows), by_group(16, width // 2), by_group(16, width // 2), whole(g_k), whole(cos_t), whole(sin_t)],
            out_specs=[by_group(rows, width // 2), by_group(rows, width // 2), by_group(16, HEAD), pl.BlockSpec((8, HEAD), lambda i, l: (0, 0))],
            scratch_shapes=[pltpu.VMEM((group, rows, width // 2), BF)]),
        out_shape=[jax.ShapeDtypeStruct((n_seq, rows, width // 2), BF)] * 2 + [jax.ShapeDtypeStruct((n_seq, 16, HEAD), F32), jax.ShapeDtypeStruct((8, HEAD), F32)],
        compiler_params=pltpu.CompilerParams(dimension_semantics=("arbitrary",), vmem_limit_bytes=VMEM),
        cost_estimate=pl.CostEstimate(flops=20 * 1000 * n_seq * rows * width // 8, bytes_accessed=n_seq * rows * width * 4, transcendentals=0),
        name="attn_bwd" + str(rows),
    )(lens, kv, rot, prob, qbd, dobd, g_k, cos_t, sin_t)


def dx_body(group, n_seq, sizes, order_ref, lens_ref, dk_ref, dv_ref, dk2_ref, dv2_ref, wk_ref, wv_ref, wk2_ref, wv2_ref, h_ref, gin_ref, dxl_ref, dhm_ref, out_ref, dgin_ref, dx_ref):
    step = pl.program_id(0)
    rows, model = h_ref.shape[1], h_ref.shape[2]
    kv_half = dk_ref.shape[2]
    inner = lax.rem(step, group)
    turn_in = lax.rem(step // group, 2)
    part_cols = model // group
    wide_cols = min(part_cols, 512)

    @pl.when(step == 0)
    def _():
        dgin_ref[...] = jnp.zeros_like(dgin_ref)

    def multiply(k_ref, v_ref, key_w, val_w, add, size):
        for j in range(part_cols // wide_cols):
            cols = pl.ds(pl.multiple_of(inner * part_cols + j * wide_cols, wide_cols), wide_cols)
            d_keys = k_ref[:, :size, :].reshape(group * size, kv_half)
            d_vals = v_ref[:, :size, :].reshape(group * size, kv_half)
            part = lax.dot_general(d_keys, key_w[cols, :], NT, preferred_element_type=F32)
            part = part + lax.dot_general(d_vals, val_w[cols, :], NT, preferred_element_type=F32)
            part = part.reshape(group, size, wide_cols)
            dx_ref[turn_in, :, :size, cols] = dx_ref[turn_in, :, :size, cols] + part if add else part

    def finish(size):
        slot = 1 - turn_in
        last = lens_ref[step - group] - 1
        dx_ref[slot, inner, pl.ds(last, 1), :] += dxl_ref[0]
        chunk = 32
        tiles = [slice(t, t + HEAD) for t in range(0, model, HEAD)]

        def finish_chunk(c, carry):
            start = pl.multiple_of(c * chunk, chunk)
            here = pl.ds(start, chunk)
            at_last = lax.broadcasted_iota(jnp.int32, (chunk, HEAD), 0) + start == last
            squares, cross = jnp.zeros((chunk, HEAD), F32), jnp.zeros((chunk, HEAD), F32)
            for t in tiles:
                hid = h_ref[0, here, t].astype(F32)
                squares = squares + hid * hid
                cross = cross + hid * (dx_ref[slot, inner, here, t] * gin_ref[:, t])
            scale = lax.rsqrt(jnp.sum(squares, axis=-1, keepdims=True) / model + NORM_EPS)
            slope = scale * scale * scale * (jnp.sum(cross, axis=-1, keepdims=True) / model)
            for t in tiles:
                hid = h_ref[0, here, t].astype(F32)
                d_x = dx_ref[slot, inner, here, t] * scale
                dgin_ref[:, t] += jnp.sum((d_x * hid).reshape(chunk // 8, 8, HEAD), axis=0)
                d_hid = d_x * gin_ref[:, t] - hid * slope
                out_ref[0, here, t] = (d_hid + jnp.where(at_last, dhm_ref[0][:, t], 0.0)).astype(BF)
            return carry

        lax.fori_loop(0, size // chunk, finish_chunk, 0)
        if size < out_ref.shape[1]:
            out_ref[0, size:, :] = jnp.zeros((out_ref.shape[1] - size, model), BF)

    first = step - inner
    longest = jnp.where(step < n_seq, lens_ref[jnp.minimum(first, n_seq - group) + group - 1], 0)
    variants(longest, sizes, functools.partial(multiply, dk_ref, dv_ref, wk_ref, wv_ref, False))
    variants(longest, sizes, functools.partial(multiply, dk2_ref, dv2_ref, wk2_ref, wv2_ref, True))
    pl.when(step >= group)(lambda: variants(lens_ref[jnp.maximum(first - group, 0) + group - 1], sizes, finish))


def attn_dx(hid, order, lens, rows, group, sizes, d_own, d_oth, w_own, w_oth, g_in, d_xlast, d_hmid):
    n_seq, seq_len, model = hid.shape
    width = 2 * w_own[0].shape[1]
    weights = tuple(w_own) + tuple(w_oth)
    once = dict(pipeline_mode=pl.Buffered(buffer_count=1))
    of_group = pl.BlockSpec((group, rows, width // 2), lambda i, o, l: (jnp.minimum(i // group, n_seq // group - 1), 0, 0))
    whole = lambda arr: pl.BlockSpec(arr.shape, lambda i, o, l: (0,) * arr.ndim, **once)
    late = lambda i: jnp.maximum(i - group, 0)
    one_row = pl.BlockSpec((1, 1, model), lambda i, o, l: (late(i), 0, 0))
    return pl.pallas_call(
        functools.partial(dx_body, group, n_seq, sizes),
        grid_spec=pltpu.PrefetchScalarGridSpec(
            num_scalar_prefetch=2, grid=(n_seq + group,),
            in_specs=[of_group] * 4 + [whole(w) for w in weights] + [pl.BlockSpec((1, rows, model), lambda i, o, l: (o[late(i)], 0, 0)),
                      whole(g_in), one_row, one_row],
            out_specs=[pl.BlockSpec((1, seq_len, model), lambda i, o, l: (o[late(i)], 0, 0)), pl.BlockSpec((8, model), lambda i, o, l: (0, 0))],
            scratch_shapes=[pltpu.VMEM((2, group, rows, model), F32)]),
        out_shape=[jax.ShapeDtypeStruct(hid.shape, BF), jax.ShapeDtypeStruct((8, model), F32)],
        compiler_params=pltpu.CompilerParams(dimension_semantics=("arbitrary",), vmem_limit_bytes=VMEM),
        cost_estimate=pl.CostEstimate(flops=4 * n_seq * rows * model * width, bytes_accessed=hid.size * 4, transcendentals=0),
        name="attn_dx" + str(rows),
    )(order, lens, *d_own, *d_oth, *weights, hid, g_in, d_xlast[:, None, :], d_hmid[:, None, :])


def wide(values):
    return values.astype(F32)


def narrow(values, unit):
    return (values * unit).astype(BF)


def swap_tp(values):
    return lax.ppermute(values, 'tp', SWAP)


def psum_tp(values):
    return values + swap_tp(values)


def psum_tp_over(values, beside):
    arrived, beside = lax.optimization_barrier((swap_tp(values), beside))
    return values + arrived, beside


def swiglu(gate_in, up_in):
    return jax.nn.silu(gate_in) * up_in


def final_head(h_out, g_final):
    z_norm = norm_rows(h_out, g_final)
    return z_norm * lax.rsqrt(jnp.sum(z_norm * z_norm, axis=-1, keepdims=True))


def dot(a, b):
    return jnp.dot(a, b, preferred_element_type=F32)


def dot_nt(a, b):
    return lax.dot_general(a, b, NT, preferred_element_type=F32)


def dot_tn(a, b):
    return lax.dot_general(a, b, TN, preferred_element_type=F32)


Q_SIZES = (32, 64, 96, 128)
D_SIZES = (128, 256, 384, 512)


def solution(mesh):
    dp_size = mesh.shape['dp']

    def device_step(hid_q, hid_d, len_q, len_d, pos_doc, w_q, w_k, w_v, w_o, w_gate, w_up, w_down, g_in, g_q, g_k, g_post, g_final):
        g_in, g_q, g_k, g_post, g_final = (gain.astype(F32) for gain in (g_in, g_q, g_k, g_post, g_final))
        n_q, n_d = hid_q.shape[0], hid_d.shape[0]
        seq_len = hid_q.shape[1]
        n_query = n_q * dp_size

        ids = jnp.arange(n_q)
        before = (len_q[None, :] < len_q[:, None]) | ((len_q[None, :] == len_q[:, None]) & (ids[None, :] < ids[:, None]))
        rank = jnp.sum(before, axis=1)
        is_rank = rank[None, :] == ids[:, None]
        order_q = jnp.sum(jnp.where(is_rank, ids[None, :], 0), axis=1).astype(jnp.int32)
        lens_q = jnp.sum(jnp.where(is_rank, len_q[None, :], 0), axis=1).astype(jnp.int32)
        pos_sorted = jnp.sum(jnp.where(is_rank, pos_doc[None, :], 0), axis=1).astype(jnp.int32)
        order_d = jnp.arange(n_d, dtype=jnp.int32)
        lens = jnp.concatenate([lens_q, len_d])
        unit = jnp.minimum(len_d[0], 1).astype(F32)

        kv_half = w_k.shape[1]
        slab_rows = w_k.shape[0] // dp_size
        my_slab = lambda arr: lax.dynamic_slice_in_dim(arr, lax.axis_index('dp') * slab_rows, slab_rows, axis=0)
        slab = jnp.concatenate([my_slab(w_k), my_slab(w_v)], axis=1)
        slab2 = swap_tp(wide(slab))

        h_last = jnp.concatenate([hid_q[order_q, lens_q - 1], hid_d[order_d, len_d - 1]], axis=0).astype(F32)
        x_last = norm_rows(h_last, g_in).astype(BF)
        q_raw = dot(x_last, w_q).astype(BF)
        q_cos, q_sin = rope_tables(lens - 1)
        q_rot, q_pull = jax.vjp(lambda raw, gain: rotate_query(raw, gain, q_cos, q_sin), q_raw, g_q)
        q_rot2 = narrow(swap_tp(wide(q_rot)), unit)
        qbd, qbd2 = block_diag(q_rot), block_diag(q_rot2)

        cos_t, sin_t = rope_tables(jnp.arange(seq_len))
        cos_q, sin_q = cos_t[:Q_MAX], sin_t[:Q_MAX]
        gin_row, gk_row = g_in[None, :], g_k[None, :]
        x_d, kv_d, p_d, o_d, rot_d = attn_fwd(hid_d, order_d, len_d, seq_len, 1, D_SIZES, w_k, w_v, qbd[n_q:], gk_row, cos_t, sin_t, gin_row)
        slab2, x_d = lax.optimization_barrier((slab2, x_d))
        w_kv2 = lax.all_gather(slab2, 'dp', axis=0, tiled=True)
        x_q, kv_q, p_q, o_q, rot_q = attn_fwd(hid_q, order_q, lens_q, Q_MAX, 4, Q_SIZES, w_k, w_v, qbd[:n_q], gk_row, cos_q, sin_q, gin_row)
        attn_out = jnp.concatenate([o_q, o_d], axis=0)[:, :q_rot.shape[1]].astype(BF).reshape(n_q + n_d, -1)

        h_mid = h_last + psum_tp(dot(attn_out, w_o))
        y_norm = norm_rows(h_mid, g_post).astype(BF)
        width = h_last.shape[1]
        pad_rows = -(n_q + n_d) % 8
        gather = lambda arr: narrow(lax.all_gather(wide(jnp.pad(arr, ((0, pad_rows), (0, 0)))), 'dp', axis=0, tiled=True), unit)
        y_norm, w_kv2 = lax.optimization_barrier((y_norm, w_kv2))
        w_kv2 = narrow(w_kv2, unit)
        w_k2, w_v2 = w_kv2[:, :kv_half], w_kv2[:, kv_half:]
        gate_val = dot(y_norm, w_gate).astype(BF)
        up_val = dot(y_norm, w_up).astype(BF)
        hidden_act, act_pull = jax.vjp(swiglu, gate_val.astype(F32), up_val.astype(F32))
        hidden_act = hidden_act.astype(BF)
        early = gather(jnp.concatenate([x_last, y_norm, attn_out, hidden_act], axis=1))
        kv2_d, p2_d, _, rot2_d = attn_fwd(x_d, order_d, len_d, seq_len, 1, D_SIZES, w_k2, w_v2, qbd2[n_q:], gk_row, cos_t, sin_t)
        mlp_out, p2_d = psum_tp_over(dot(hidden_act, w_down), p2_d)
        h_out = h_mid + mlp_out
        emb, head_pull = jax.vjp(final_head, h_out, g_final)
        emb_q, emb_d = emb[:n_q], emb[n_q:]

        all_docs = lax.all_gather(emb_d, 'dp', axis=0, tiled=True)
        logits = jnp.einsum('qd,kd->qk', emb_q, all_docs, precision=lax.Precision.HIGHEST) / TEMPERATURE
        log_norm = jax.nn.logsumexp(logits, axis=1)
        is_pos = jnp.arange(all_docs.shape[0])[None, :] == pos_sorted[:, None]
        loss_sorted = log_norm - jnp.sum(jnp.where(is_pos, logits, 0.0), axis=1)
        loss_rows = jnp.sum(jnp.where(is_rank, loss_sorted[:, None], 0.0), axis=0)
        d_logits = (jnp.exp(logits - log_norm[:, None]) - is_pos.astype(F32)) / (n_query * TEMPERATURE)
        d_emb_q = jnp.einsum('qk,kd->qd', d_logits, all_docs, precision=lax.Precision.HIGHEST)
        d_docs = jnp.einsum('qk,qd->kd', d_logits, emb_q, precision=lax.Precision.HIGHEST)
        d_docs = lax.all_to_all(d_docs, 'dp', 0, 0, tiled=True)
        d_emb_d = jnp.sum(d_docs.reshape(dp_size, n_d, width), axis=0)

        d_hout, d_gfinal = head_pull(jnp.concatenate([d_emb_q, d_emb_d], axis=0))
        d_hout_b = d_hout.astype(BF)
        d_act = dot_nt(d_hout_b, w_down).astype(BF)
        d_gate, d_up = (d_in.astype(BF) for d_in in act_pull(d_act.astype(F32)))
        kv2_q, p2_q, _, rot2_q = attn_fwd(x_q, order_q, lens_q, Q_MAX, 4, Q_SIZES, w_k2, w_v2, qbd2[:n_q], gk_row, cos_q, sin_q)
        d_y, p2_q = psum_tp_over(dot_nt(d_gate, w_gate) + dot_nt(d_up, w_up), p2_q)
        d_ymid, d_gpost = norm_back(h_mid, g_post, d_y)
        d_hmid = d_hout + d_ymid
        d_hmid_b = d_hmid.astype(BF)
        d_hmid_b, early = lax.optimization_barrier((d_hmid_b, early))
        d_both = gather(jnp.concatenate([d_hout_b, d_hmid_b, d_gate, d_up], axis=1))
        d_attn = dot_nt(d_hmid_b, w_o).astype(BF).reshape(q_rot.shape)
        d_attn2 = narrow(swap_tp(wide(d_attn)), unit)
        dobd, dobd2 = block_diag(d_attn), block_diag(d_attn2)

        dk_q, dv_q, dq_q, dgk_q = attn_bwd(lens_q, 4, Q_SIZES, kv_q, rot_q, p_q, qbd[:n_q], dobd[:n_q], gk_row, cos_q, sin_q)
        dk_d, dv_d, dq_d, dgk_d = attn_bwd(len_d, 1, D_SIZES, kv_d, rot_d, p_d, qbd[n_q:], dobd[n_q:], gk_row, cos_t, sin_t)
        d_qrot = jnp.concatenate([dq_q, dq_d], axis=0)[:, :q_rot.shape[1]].astype(BF)
        d_qraw, d_gq = q_pull(d_qrot)
        d_xlast = psum_tp(dot_nt(d_qraw, w_q))
        flat = lambda arr: arr.reshape(-1, arr.shape[-1])
        d_wk = dot_tn(flat(x_q), flat(dk_q)) + dot_tn(flat(x_d), flat(dk_d))
        d_wv = dot_tn(flat(x_q), flat(dv_q)) + dot_tn(flat(x_d), flat(dv_d))
        d_wk, d_wv, d_both = lax.optimization_barrier((d_wk, d_wv, d_both))
        d_wk, d_wv = lax.psum((d_wk, d_wv), 'dp')

        dk2_q, dv2_q, _, _ = attn_bwd(lens_q, 4, Q_SIZES, kv2_q, rot2_q, p2_q, qbd2[:n_q], dobd2[:n_q], gk_row, cos_q, sin_q)
        dk2_d, dv2_d, _, _ = attn_bwd(len_d, 1, D_SIZES, kv2_d, rot2_d, p2_d, qbd2[n_q:], dobd2[n_q:], gk_row, cos_t, sin_t)
        d_hid_q, dgin_q = attn_dx(hid_q, order_q, lens_q, Q_MAX, 4, Q_SIZES, (dk_q, dv_q), (dk2_q, dv2_q), (w_k, w_v), (w_k2, w_v2), gin_row, d_xlast[:n_q], d_hmid[:n_q])
        d_hid_d, dgin_d = attn_dx(hid_d, order_d, len_d, seq_len, 1, D_SIZES, (dk_d, dv_d), (dk2_d, dv2_d), (w_k, w_v), (w_k2, w_v2), gin_row, d_xlast[n_q:], d_hmid[n_q:])

        d_qraw, d_wk, d_wv, dgin_q = lax.optimization_barrier((d_qraw, d_wk, d_wv, dgin_q))
        d_qraw_all = gather(d_qraw)
        kv_width = attn_out.shape[1]
        x_last_all, y_all = early[:, :width], early[:, width:2 * width]
        attn_all, act_all = early[:, 2 * width:2 * width + kv_width], early[:, 2 * width + kv_width:]
        d_hout_all, d_hmid_all = d_both[:, :width], d_both[:, width:2 * width]
        d_gate_all, d_up_all = jnp.split(d_both[:, 2 * width:], 2, axis=1)
        d_wdown = dot_tn(act_all, d_hout_all)
        d_wgate = dot_tn(y_all, d_gate_all)
        d_wup = dot_tn(y_all, d_up_all)
        d_wo = dot_tn(attn_all, d_hmid_all)
        d_wq = dot_tn(x_last_all, d_qraw_all)

        dp_sum = lambda vec: jnp.sum(lax.all_gather(vec, 'dp', axis=0), axis=0)
        d_heads = psum_tp(jnp.concatenate([d_gq, jnp.sum(dgk_q + dgk_d, axis=0)]))
        gains = dp_sum(jnp.concatenate([d_gpost, d_gfinal, jnp.sum(dgin_q + dgin_d, axis=0), d_heads]))
        d_gpost, d_gfinal, d_gin, d_heads = jnp.split(gains, (width, 2 * width, 3 * width))
        d_gq, d_gk = d_heads[:HEAD], d_heads[HEAD:]
        return (loss_rows, d_hid_q, d_hid_d, d_wq, d_wk, d_wv, d_wo, d_wgate, d_wup, d_wdown,
                d_gin, d_gq, d_gk, d_gpost, d_gfinal)

    col_split = P(None, 'tp')
    row_split = P('tp', None)
    in_specs = (P('dp'), P('dp'), P('dp'), P('dp'), P('dp'), col_split, col_split, col_split, row_split, col_split, col_split, row_split, P(), P(), P(), P(), P())
    out_specs = (P('dp'), P('dp'), P('dp'), col_split, col_split, col_split, row_split, col_split, col_split, row_split, P(), P(), P(), P(), P())
    return jax.shard_map(device_step, mesh=mesh, in_specs=in_specs, out_specs=out_specs, check_vma=False)
```
